256 devices in a mesh: dp: 32 (over y_hi, z, core), vocab: 8 (over x, y_lo).
Axes of the slice: x: 4, y: 4 (y_hi: 2, y_lo: 2; y = y_hi * 2 + y_lo), z: 8, core: 2. Of those that a mesh axis runs over, the one named last changes fastest.
Arguments:
- hidden: bfloat16 [16384, 3072], P(('dp', 'vocab')), may hold values from -128 to 128
- targets: int32 [16384], P(('dp', 'vocab')), may hold values from 0 to 16383
- lengths: int32 [32], P('dp'), may hold values from 1 to 512
- head: bfloat16 [3072, 16384], P('dp', 'vocab'), may hold values from -1 to 1
Outputs:
- grad_hidden: bfloat16 [16384, 3072], P(('dp', 'vocab'))
- loss: float32 [], replicated
The draws below stay inside these ranges and needn't reach their ends.
All inputs are finite; a program needn't handle non-finite values.
Results may differ from the reference program's by a relative error of at most 0.0052.
Values may be sent and summed in bfloat16 or wider, within the bound.
A program may use at most 64 MiB of HBM per device.

```python
import jax
import jax.numpy as jnp
from jax import lax

D = 3072
CLIP = 512
LEVELS = 16384
TOKENS = 16384
N_DP = 32


def head_values(key):
    base_key = jax.random.fold_in(key, 11)
    values = jax.random.normal(base_key, (D, LEVELS), jnp.float32) * (3.0 / D ** 0.5)
    return jnp.clip(values, -1.0, 1.0)


def draw_head(key, part):
    return head_values(key).astype(jnp.bfloat16)


def draw_hidden(key, part):
    values = jnp.clip(jax.random.normal(jax.random.fold_in(key, 23), (TOKENS, D), jnp.float32), -6.0, 6.0)
    return values.astype(jnp.bfloat16)


def plant(result, stream_key, smallest, high):
    longest = result.shape.index(max(result.shape))
    spots = []
    for shift in (0, 1):
        where = [jax.random.randint(jax.random.fold_in(stream_key, axis), (), 0, length) for axis, length in enumerate(result.shape)]
        where[longest] = (where[longest] + shift) % result.shape[longest]
        spots.append(tuple(where))
    return result.at[spots[0]].set(smallest).at[spots[1]].set(high)


def setup_inputs(seed: int = 0) -> dict:
    splits = jax.random.split(jax.random.key(seed), 5)
    return {
        "hidden": draw_hidden(jax.random.fold_in(splits[4], 71), 0),
        "targets": plant(jax.random.randint(splits[1], (TOKENS,), 0, LEVELS), jax.random.fold_in(splits[1], 1), 0, LEVELS - 1).astype(jnp.int32),
        "lengths": plant(jax.random.randint(splits[2], (N_DP,), 1, CLIP + 1), jax.random.fold_in(splits[2], 1), 1, CLIP).astype(jnp.int32),
        "head": draw_head(jax.random.fold_in(splits[4], 71), 0),
    }


def clip_terms(clip_rows, clip_targets, clip_length, head, total_count):
    logits = jnp.dot(clip_rows, head, preferred_element_type=jnp.float32)
    maxima = jnp.max(logits, axis=1)
    totals = jnp.sum(jnp.exp(logits - maxima[:, None]), axis=1)
    log_total = maxima + jnp.log(totals)
    level_grid = jnp.arange(head.shape[1], dtype=jnp.int32)
    is_target = clip_targets[:, None] == level_grid[None, :]
    target_logit = jnp.sum(jnp.where(is_target, logits, 0.0), axis=1)
    positions = jnp.arange(clip_rows.shape[0], dtype=jnp.int32)
    valid_rows = (positions < clip_length).astype(jnp.float32)
    loss_sum = jnp.sum(valid_rows * (log_total - target_logit))
    weights = (valid_rows / total_count)[:, None]
    grad_logits = (weights * (jnp.exp(logits - log_total[:, None]) - is_target.astype(jnp.float32))).astype(jnp.bfloat16)
    grad_rows = lax.dot_general(grad_logits, head, (((1,), (1,)), ((), ())), preferred_element_type=jnp.float32)
    return grad_rows.astype(jnp.bfloat16), loss_sum


def reference(hidden, targets, lengths, head):
    total_count = jnp.sum(lengths).astype(jnp.float32)

    def one_clip(clip_items):
        return clip_terms(clip_items[0], clip_items[1], clip_items[2], head, total_count)

    grad_blocks, loss_sums = lax.map(one_clip, (hidden.reshape(N_DP, CLIP, D), targets.reshape(N_DP, CLIP), lengths))
    return grad_blocks.reshape(TOKENS, D), jnp.sum(loss_sums) / total_count
```

```python
import jax
import jax.numpy as jnp
from jax import lax
from jax.experimental import pallas as pl
from jax.experimental.pallas import tpu as pltpu
from jax.sharding import Mesh
from jax.sharding import PartitionSpec as P

AXES = ("yh", "z", "c", "x", "yl")
SIZES = (2, 8, 2, 4, 2)
DP = ("yh", "z", "c")
VOCAB = ("x", "yl")
MESH = pl.DeviceIdType.MESH

WIDTH = 3072
LEVELS = 2048
HOME = 64
ROWS = 512
HEAD_ROWS = 96
PART = 48
HALF = LEVELS // 2
CHUNKS = 6
CHUNK = WIDTH // CHUNKS
PAIR = 384


def kernel(
    hid_ref, aux_ref, head_ref, grad_ref, loss_ref,
    H, X, A, L, G, PT, R1, R2, R3, S2, SY, YR, KEEP, ST, LS, SB,
    zs, zr, ys, yr, cs, cr, hs, hr, as_, ar, ts, tr, ss, sr, rs, rr, ls,
):
    yh, z, c, x, yl = (lax.axis_index(name) for name in AXES)
    oyh, oc, oyl = 1 - yh, 1 - c, 1 - yl
    me = x * 2 + yl

    def remote(src, dst, send, recv, **device):
        return pltpu.make_async_remote_copy(
            src_ref=src, dst_ref=dst, send_sem=send, recv_sem=recv,
            device_id=device, device_id_type=MESH,
        )

    def zdev(d):
        return lax.rem(z + d + 8, 8)

    def xdev(d):
        return lax.rem(x + d + 4, 4)

    vocab_peers = [(dx, dy) for dx in range(4) for dy in range(2) if dx or dy]

    def vpeer(dx, dy):
        return dict(x=xdev(dx), yl=lax.rem(yl + dy, 2))

    def vindex(dx, dy):
        return xdev(-dx) * 2 + lax.rem(yl + dy, 2)

    barrier = pltpu.get_barrier_semaphore()
    peers = [dict(c=oc), dict(yh=oyh)]
    peers += [dict(z=zdev(d)) for d in range(1, 8)]
    peers += [vpeer(dx, dy) for dx, dy in vocab_peers]
    for device in peers:
        pl.semaphore_signal(barrier, 1, device_id=device, device_id_type=MESH)

    def row0(ring, zz, cc):
        return ring * 1536 + zz * 192 + cc * 96

    def head_at(ring, zz, cc, start, size, lanes=None):
        rows = pl.ds(pl.multiple_of(row0(ring, zz, cc) + start, 16), size)
        if lanes is None:
            return H.at[rows, :]
        return H.at[rows, pl.ds(lanes * HALF, HALF)]

    own_copies = [
        pltpu.make_async_copy(head_ref, head_at(yh, z, c, 0, HEAD_ROWS), ls.at[0]),
        pltpu.make_async_copy(hid_ref, X.at[pl.ds(pl.multiple_of(me * HOME, HOME), HOME), :], ls.at[1]),
        pltpu.make_async_copy(aux_ref, A.at[me], ls.at[2]),
    ]
    for copy in own_copies:
        copy.start()
    SB[0, 0] = jnp.broadcast_to(aux_ref[1:2, :].astype(jnp.float32), (8, 128))
    pl.semaphore_wait(barrier, len(peers))

    sent = []

    def send(copy):
        copy.start()
        sent.append(copy)

    def sum_copy(k, stage, d=0):
        if stage == 0:
            return remote(SB.at[k, 0], SB.at[k, 1], ss.at[k, 0], sr.at[k, 0], c=oc)
        if stage == 1:
            return remote(SB.at[k, 2], SB.at[k, 3], ss.at[k, 1], sr.at[k, 1], yh=oyh)
        return remote(
            SB.at[k, 4 + z], SB.at[k, 4 + z], ss.at[k, 1 + d], sr.at[k, 1 + d], z=zdev(d)
        )

    def sum_stage(k, stage):
        if stage == 1:
            sum_copy(k, 0).wait_recv()
            SB[k, 2] = SB[k, 0] + SB[k, 1]
            sum_copy(k, 1).start()
        elif stage == 2:
            sum_copy(k, 1).wait_recv()
            SB[k, 4 + z] = SB[k, 2] + SB[k, 3]
            for d in range(1, 8):
                sum_copy(k, 2, d).start()
        elif stage == 3:
            for d in range(1, 8):
                remote(
                    SB.at[k, 4 + z], SB.at[k, 4 + zdev(-d)], ss.at[k, 1 + d], sr.at[k, 1 + d], z=zdev(d)
                ).wait_recv()
            total = SB[k, 4]
            for n in range(1, 8):
                total = total + SB[k, 4 + n]
            for stage_ in range(2):
                sum_copy(k, stage_).wait_send()
            for d in range(1, 8):
                sum_copy(k, 2, d).wait_send()
            return total

    DIRS = (1, -1)
    B, OWN_A, PEER_A = 0, 1, 2

    def item_at(item, zz, cc, lanes=None):
        if item == B:
            return head_at(yh, zz, cc, PART, PART, lanes)
        return head_at(yh if item == OWN_A else oyh, zz, cc, 0, PART, lanes)

    def lanes_of(step, dr):
        return None if step < 4 else (0 if dr == 0 else 1)

    def z_send(item, step, dr, src=None):
        zz = zdev(-DIRS[dr] * (step - 1))
        there = item_at(item, zz, c, lanes_of(step, dr))
        send(remote(
            there if src is None else src, there,
            zs.at[dr, step - 1, item], zr.at[dr, step - 1, item], z=zdev(DIRS[dr]),
        ))

    def z_wait(item, step, dr):
        here = item_at(item, zdev(-DIRS[dr] * step), c, lanes_of(step, dr))
        remote(
            here, here, zs.at[dr, step - 1, item], zr.at[dr, step - 1, item], z=zdev(DIRS[dr])
        ).wait_recv()
        return here

    def c_send(index, ref, src=None):
        send(remote(ref if src is None else src, ref, cs.at[index], cr.at[index], c=oc))

    def c_wait(index, ref):
        remote(ref, ref, cs.at[index], cr.at[index], c=oc).wait_recv()

    def c_index(item, step, dr):
        return 1 + (dr * 4 + step - 1) * 3 + item

    def y_send(index, ref, src=None):
        send(remote(ref if src is None else src, ref, ys.at[index], yr.at[index], yh=oyh))

    def y_wait(index, ref):
        remote(ref, ref, ys.at[index], yr.at[index], yh=oyh).wait_recv()

    def y_index(step, dr):
        return 2 + dr * 4 + step - 1

    def peer_b(step, dr, cc):
        return head_at(oyh, zdev(-DIRS[dr] * step), cc, PART, PART, lanes_of(step, dr))

    def hid_at(v, half=None):
        if half is None:
            return X.at[pl.ds(pl.multiple_of(v * HOME, HOME), HOME), :]
        return X.at[pl.ds(pl.multiple_of(v * HOME + half * 32, 32), 32), :]

    sum_copy(0, 0).start()
    for n, (dx, dy) in enumerate(vocab_peers):
        send(remote(aux_ref, A.at[me], as_.at[n], ar.at[n], **vpeer(dx, dy)))
    own_a, own_b = head_ref.at[pl.ds(0, PART), :], head_ref.at[pl.ds(PART, PART), :]
    send(remote(hid_ref, hid_at(me), hs.at[0], hr.at[0], yl=oyl))
    y_send(0, head_at(yh, z, c, 0, PART), own_a)
    for dr in range(2):
        z_send(B, 1, dr, own_b)
        send(remote(hid_ref, hid_at(me), hs.at[1 + dr], hr.at[1 + dr], x=xdev(DIRS[dr])))
    y_send(1, head_at(yh, z, c, PART, PART), own_b)
    for dr in range(2):
        z_send(OWN_A, 1, dr, own_a)
    c_send(0, head_at(yh, z, c, 0, HEAD_ROWS), head_ref)

    ref = head_at(oyh, z, c, 0, PART)
    y_wait(0, ref)
    for dr in range(2):
        z_send(PEER_A, 1, dr)
    c_send(25, ref)
    hid_peer = hid_at(x * 2 + oyl)
    remote(hid_peer, hid_peer, hs.at[0], hr.at[0], yl=oyl).wait_recv()
    for dr in range(2):
        send(remote(hid_peer, hid_peer, hs.at[3 + dr], hr.at[3 + dr], x=xdev(DIRS[dr])))
    ref = head_at(oyh, z, c, PART, PART)
    y_wait(1, ref)
    c_send(26, ref)
    sum_stage(0, 1)

    def pass_on(items, step):
        for item in items:
            for dr in range(2):
                here = z_wait(item, step, dr)
                if step < 4:
                    z_send(item, step + 1, dr)
                if item == B:
                    y_send(y_index(step, dr), here)
                c_send(c_index(item, step, dr), here)

    def take_y(step):
        for dr in range(2):
            ref = peer_b(step, dr, c)
            y_wait(y_index(step, dr), ref)
            c_send(27 + dr * 4 + step - 1, ref)

    def take_c(step):
        for dr in range(2):
            for item in range(3):
                c_wait(
                    c_index(item, step, dr),
                    item_at(item, zdev(-DIRS[dr] * step), oc, lanes_of(step, dr)),
                )
            c_wait(27 + dr * 4 + step - 1, peer_b(step, dr, oc))

    def hid_pass(kind):
        for dr in range(2):
            v = xdev(-DIRS[dr]) * 2 + (yl if kind == 0 else oyl)
            ref = hid_at(v)
            n = 1 + 2 * kind + dr
            remote(ref, ref, hs.at[n], hr.at[n], x=xdev(DIRS[dr])).wait_recv()
            half = hid_at(v, dr)
            n = 5 + 2 * kind + dr
            send(remote(half, half, hs.at[n], hr.at[n], x=xdev(DIRS[dr])))

    def hid_far(kind):
        for dr in range(2):
            half = hid_at(xdev(2) * 2 + (yl if kind == 0 else oyl), dr)
            n = 5 + 2 * kind + dr
            remote(half, half, hs.at[n], hr.at[n], x=xdev(DIRS[dr])).wait_recv()

    def multiply(q, first=False):
        pair = lax.rem(lax.div(z, 2) + q, 4)
        for ring in range(2):
            start = pl.multiple_of(ring * 1536 + pair * PAIR, 128)

            def tile(n, carry, start=start, fresh=first and ring == 0):
                at = pl.ds(pl.multiple_of(n * 256, 256), 256)
                part = jnp.dot(
                    X[:, pl.ds(start, PAIR)], H[pl.ds(start, PAIR), at],
                    preferred_element_type=jnp.float32,
                )
                if fresh:
                    L[:, at] = part
                else:
                    L[:, at] += part
                return carry

            lax.fori_loop(0, LEVELS // 256, tile, 0)

    pass_on((B, OWN_A, PEER_A), 1)
    hid_pass(0)
    pass_on((B, OWN_A, PEER_A), 2)
    take_y(1)
    hid_pass(1)
    sum_stage(0, 2)
    pass_on((B, OWN_A, PEER_A), 3)
    take_y(2)
    for copy in own_copies:
        copy.wait()
    c_wait(0, head_at(yh, z, oc, 0, HEAD_ROWS))
    c_wait(25, head_at(oyh, z, oc, 0, PART))
    c_wait(26, head_at(oyh, z, oc, PART, PART))
    take_c(1)
    hid_far(0)
    hid_far(1)
    for n, (dx, dy) in enumerate(vocab_peers):
        there = A.at[vindex(dx, dy)]
        remote(aux_ref, there, as_.at[n], ar.at[n], **vpeer(dx, dy)).wait_recv()
    multiply(0, first=True)
    take_y(3)
    take_c(2)
    take_c(3)
    multiply(1)
    pass_on((B,), 4)
    multiply(3)
    pass_on((OWN_A, PEER_A), 4)
    take_y(4)
    count_tile = sum_stage(0, 3)
    take_c(4)
    multiply(2)

    base = me * LEVELS
    lane = lax.broadcasted_iota(jnp.int32, (HOME, 128), 1)
    eye = lane == lax.broadcasted_iota(jnp.int32, (HOME, 128), 0)
    level = lax.broadcasted_iota(jnp.int32, (HOME, LEVELS), 1)

    def to_row(column):
        return jnp.sum(jnp.where(eye, column, 0.0), axis=0, keepdims=True)

    def to_column(row):
        return jnp.sum(jnp.where(eye, row, 0.0), axis=1, keepdims=True)

    def target_of(v):
        row = A[v][0:1, :].astype(jnp.float32)
        return to_column(row).astype(jnp.int32) - base

    def rows_of(v):
        return pl.ds(pl.multiple_of(v * HOME, HOME), HOME)

    def statistics(v, carry):
        logits = L[rows_of(v), :]
        top = jnp.max(logits, axis=1, keepdims=True)
        total = jnp.sum(jnp.exp(logits - top), axis=1, keepdims=True)
        hit = jnp.sum(jnp.where(level == target_of(v), logits, 0.0), axis=1, keepdims=True)
        for n, column in enumerate((top, total, hit)):
            ST[me, n, pl.ds(v, 1), :] = to_row(column)
        return carry

    lax.fori_loop(0, 8, statistics, 0)
    for n, (dx, dy) in enumerate(vocab_peers):
        send(remote(ST.at[me], ST.at[me], ts.at[n], tr.at[n], **vpeer(dx, dy)))
    for n, (dx, dy) in enumerate(vocab_peers):
        there = ST.at[vindex(dx, dy)]
        remote(ST.at[me], there, ts.at[n], tr.at[n], **vpeer(dx, dy)).wait_recv()

    top = ST[0, 0]
    for v in range(1, 8):
        top = jnp.maximum(top, ST[v, 0])
    total = jnp.zeros((8, 128), jnp.float32)
    hit = jnp.zeros((8, 128), jnp.float32)
    for v in range(8):
        total = total + ST[v, 1] * jnp.exp(ST[v, 0] - top)
        hit = hit + ST[v, 2]
    log_total = top + jnp.log(total)
    LS[...] = log_total

    length = aux_ref[1:2, 0:1]
    lane8 = lax.broadcasted_iota(jnp.int32, (8, 128), 1)
    place = lax.broadcasted_iota(jnp.int32, (8, 128), 0) * HOME + lane8
    counted = (lane8 < HOME) & (place < length)
    row_loss = jnp.where(counted, log_total - hit, 0.0)
    clip_loss = jnp.sum(jnp.sum(row_loss, axis=1, keepdims=True), axis=0, keepdims=True)
    SB[1, 0] = jnp.broadcast_to(clip_loss, (8, 128))
    count = count_tile[0:1, 0:1]

    def gradient(v, carry):
        place = v * HOME + lax.broadcasted_iota(jnp.int32, (HOME, 1), 0)
        weight = jnp.where(place < length, 1.0, 0.0) / count
        share = jnp.exp(L[rows_of(v), :] - to_column(LS[pl.ds(v, 1), :]))
        share = share - jnp.where(level == target_of(v), 1.0, 0.0)
        G[rows_of(v), :] = (weight * share).astype(jnp.bfloat16)
        return carry

    lax.fori_loop(0, 8, gradient, 0)
    sum_copy(1, 0).start()

    def block(j, xx):
        return PT.at[j, pl.ds(pl.multiple_of(xx * 128, 128), 128), :]

    def scatter(j, kind):
        d = 1 - 2 * lax.rem(j, 2)
        if kind == 0:
            return remote(block(j, xdev(2)), R1.at[j], rs.at[0, j], rr.at[0, j], x=xdev(d))
        if kind == 1:
            return remote(block(j, xdev(-d)), R2.at[j], rs.at[1, j], rr.at[1, j], x=xdev(-d))
        if kind == 2:
            return remote(S2.at[j], R3.at[j], rs.at[2, j], rr.at[2, j], x=xdev(d))
        return remote(SY.at[j], YR.at[j], rs.at[3, j], rr.at[3, j], yl=oyl)

    def f32(value):
        return value.astype(jnp.float32)

    def scatter_step(j, carry):
        @pl.when(j < CHUNKS)
        def _():
            for n in range(2):
                rows = pl.ds(pl.multiple_of(j * CHUNK + n * 256, 256), 256)
                PT[j, :, n * 256 : (n + 1) * 256] = lax.dot_general(
                    G[...], H[rows, :], (((1,), (1,)), ((), ())),
                    preferred_element_type=jnp.float32,
                ).astype(jnp.bfloat16)
            scatter(j, 0).start()
            scatter(j, 1).start()

        @pl.when((j >= 1) & (j < CHUNKS + 1))
        def _():
            k = j - 1
            d = 1 - 2 * lax.rem(k, 2)
            scatter(k, 0).wait_recv()
            mine = PT[k, pl.ds(pl.multiple_of(xdev(d) * 128, 128), 128), :]
            S2[k] = (f32(R1[k]) + f32(mine)).astype(jnp.bfloat16)
            scatter(k, 2).start()

        @pl.when((j >= 2) & (j < CHUNKS + 2))
        def _():
            k = j - 2
            scatter(k, 1).wait_recv()
            scatter(k, 2).wait_recv()

            def total_of(which):
                mine = PT[k, pl.ds(pl.multiple_of(x * 128 + which * HOME, HOME), HOME), :]
                half = pl.ds(pl.multiple_of(which * HOME, HOME), HOME)
                return f32(mine) + f32(R2[k, half, :]) + f32(R3[k, half, :])

            SY[k] = total_of(oyl).astype(jnp.bfloat16)
            scatter(k, 3).start()
            KEEP[k] = total_of(yl)

        @pl.when(j >= 3)
        def _():
            k = j - 3
            scatter(k, 3).wait_recv()
            at = pl.ds(pl.multiple_of(k * CHUNK, CHUNK), CHUNK)
            grad_ref[:, at] = (KEEP[k] + f32(YR[k])).astype(jnp.bfloat16)

        @pl.when(j == 2)
        def _():
            sum_stage(1, 1)

        @pl.when(j == 4)
        def _():
            sum_stage(1, 2)

        return carry

    lax.fori_loop(0, CHUNKS + 3, scatter_step, 0)

    loss_ref[...] = sum_stage(1, 3) / count_tile
    for copy in sent:
        copy.wait_send()

    def drain(j, carry):
        for kind in range(4):
            scatter(j, kind).wait_send()
        return carry

    lax.fori_loop(0, CHUNKS, drain, 0)


def local(hidden, targets, lengths, head):
    aux = jnp.concatenate(
        [
            jnp.pad(targets, (0, 128 - HOME)).reshape(1, 128),
            jnp.broadcast_to(lengths.reshape(1, 1), (7, 128)),
        ]
    )
    bf16, f32, i32 = jnp.bfloat16, jnp.float32, jnp.int32
    vmem = pl.BlockSpec(memory_space=pltpu.VMEM)
    dma = pltpu.SemaphoreType.DMA
    grad, loss = pl.pallas_call(
        kernel,
        out_shape=(
            jax.ShapeDtypeStruct((HOME, WIDTH), bf16),
            jax.ShapeDtypeStruct((8, 128), f32),
        ),
        in_specs=[vmem] * 3,
        out_specs=(vmem, vmem),
        scratch_shapes=[
            pltpu.VMEM((WIDTH, LEVELS), bf16),
            pltpu.VMEM((ROWS, WIDTH), bf16),
            pltpu.VMEM((8, 8, 128), i32),
            pltpu.VMEM((ROWS, LEVELS), f32),
            pltpu.VMEM((ROWS, LEVELS), bf16),
            pltpu.VMEM((CHUNKS, ROWS, CHUNK), bf16),
            pltpu.VMEM((CHUNKS, 128, CHUNK), bf16),
            pltpu.VMEM((CHUNKS, 128, CHUNK), bf16),
            pltpu.VMEM((CHUNKS, 128, CHUNK), bf16),
            pltpu.VMEM((CHUNKS, 128, CHUNK), bf16),
            pltpu.VMEM((CHUNKS, HOME, CHUNK), bf16),
            pltpu.VMEM((CHUNKS, HOME, CHUNK), bf16),
            pltpu.VMEM((CHUNKS, HOME, CHUNK), f32),
            pltpu.VMEM((8, 3, 8, 128), f32),
            pltpu.VMEM((8, 128), f32),
            pltpu.VMEM((2, 12, 8, 128), f32),
            dma((2, 4, 3)), dma((2, 4, 3)),
            dma((10,)), dma((10,)),
            dma((35,)), dma((35,)),
            dma((9,)), dma((9,)),
            dma((7,)), dma((7,)),
            dma((7,)), dma((7,)),
            dma((2, 9)), dma((2, 9)),
            dma((4, CHUNKS)), dma((4, CHUNKS)),
            dma((3,)),
        ],
        compiler_params=pltpu.CompilerParams(
            collective_id=0, has_side_effects=True, vmem_limit_bytes=58 * 2**20
        ),
    )(hidden, aux, head)
    return grad, loss[0, 0]


def solution(mesh):
    torus = Mesh(mesh.devices.reshape(SIZES), AXES)
    return jax.shard_map(
        local,
        mesh=torus,
        in_specs=(P(DP + VOCAB, None), P(DP + VOCAB), P(DP), P(DP, VOCAB)),
        out_specs=(P(DP + VOCAB, None), P()),
        check_vma=False,
    )
```

```python
import jax
import jax.numpy as jnp
from jax import lax
from jax.experimental import pallas as pl
from jax.experimental.pallas import tpu as pltpu
from jax.sharding import Mesh
from jax.sharding import PartitionSpec as P

AXES = ("yh", "z", "c", "x", "yl")
SIZES = (2, 8, 2, 4, 2)
DP = ("yh", "z", "c")
VOCAB = ("x", "yl")
MESH = pl.DeviceIdType.MESH

WIDTH = 3072
LEVELS = 2048
HOME = 64
ROWS = 512
HEAD_ROWS = 96
PART = 48
HALF = LEVELS // 2
CHUNKS = 6
CHUNK = WIDTH // CHUNKS
QUAD = 768
XC, YC = 4, 2


def kernel(
    hid_ref, tgt_ref, len_ref, head_ref, grad_ref, loss_ref,
    H, X, A, L, G, PT, XR1, XR2, XR3, XS2, SY, YR, YF, SA, YR1, YR2, YR3, YS2, ST, LS, SB,
    zs, zr, ys, yr, cs, cr, hs, hr, as_, ar, ts, tr, ss, sr, xs, xr, ws, wr, ls,
):
    yh, z, c, x, yl = (lax.axis_index(name) for name in AXES)
    oyh, oc, oyl = 1 - yh, 1 - c, 1 - yl
    me = x * 2 + yl

    def remote(src, dst, send, recv, **device):
        return pltpu.make_async_remote_copy(
            src_ref=src, dst_ref=dst, send_sem=send, recv_sem=recv,
            device_id=device, device_id_type=MESH,
        )

    def zdev(d):
        return lax.rem(z + d + 8, 8)

    def xdev(d):
        return lax.rem(x + d + 4, 4)

    vocab_peers = [(dx, dy) for dx in range(4) for dy in range(2) if dx or dy]

    def vpeer(dx, dy):
        return dict(x=xdev(dx), yl=lax.rem(yl + dy, 2))

    def vindex(dx, dy):
        return xdev(-dx) * 2 + lax.rem(yl + dy, 2)

    barrier = pltpu.get_barrier_semaphore()
    peers = [dict(c=oc), dict(yh=oyh)]
    peers += [dict(z=zdev(d)) for d in range(1, 8)]
    peers += [vpeer(dx, dy) for dx, dy in vocab_peers]
    for device in peers:
        pl.semaphore_signal(barrier, 1, device_id=device, device_id_type=MESH)

    def row0(ring, zz, cc):
        return ring * 1536 + zz * 192 + cc * 96

    def head_at(ring, zz, cc, start, size, lanes=None):
        rows = pl.ds(pl.multiple_of(row0(ring, zz, cc) + start, 16), size)
        if lanes is None:
            return H.at[rows, :]
        return H.at[rows, pl.ds(lanes * HALF, HALF)]

    own_copies = [
        pltpu.make_async_copy(head_ref, head_at(yh, z, c, 0, HEAD_ROWS), ls.at[0]),
        pltpu.make_async_copy(hid_ref, X.at[pl.ds(pl.multiple_of(me * HOME, HOME), HOME), :], ls.at[1]),
        pltpu.make_async_copy(tgt_ref, A.at[me], ls.at[2]),
    ]
    for copy in own_copies:
        copy.start()
    SB[0, 0] = jnp.full((8, 128), len_ref[0], jnp.int32).astype(jnp.float32)
    pl.semaphore_wait(barrier, len(peers))

    sent = []

    def send(copy):
        copy.start()
        sent.append(copy)

    def sum_copy(k, stage, d=0):
        if stage == 0:
            return remote(SB.at[k, 0], SB.at[k, 1], ss.at[k, 0], sr.at[k, 0], c=oc)
        if stage == 1:
            return remote(SB.at[k, 2], SB.at[k, 3], ss.at[k, 1], sr.at[k, 1], yh=oyh)
        return remote(
            SB.at[k, 4 + z], SB.at[k, 4 + z], ss.at[k, 1 + d], sr.at[k, 1 + d], z=zdev(d)
        )

    def sum_stage(k, stage):
        if stage == 1:
            sum_copy(k, 0).wait_recv()
            SB[k, 2] = SB[k, 0] + SB[k, 1]
            sum_copy(k, 1).start()
        elif stage == 2:
            sum_copy(k, 1).wait_recv()
            SB[k, 4 + z] = SB[k, 2] + SB[k, 3]
            for d in range(1, 8):
                sum_copy(k, 2, d).start()
        elif stage == 3:
            for d in range(1, 8):
                remote(
                    SB.at[k, 4 + z], SB.at[k, 4 + zdev(-d)], ss.at[k, 1 + d], sr.at[k, 1 + d], z=zdev(d)
                ).wait_recv()
            total = SB[k, 4]
            for n in range(1, 8):
                total = total + SB[k, 4 + n]
            for stage_ in range(2):
                sum_copy(k, stage_).wait_send()
            for d in range(1, 8):
                sum_copy(k, 2, d).wait_send()
            return total

    DIRS = (1, -1)
    B, OWN_A, PEER_A = 0, 1, 2

    def item_at(item, zz, cc, lanes=None):
        if item == B:
            return head_at(yh, zz, cc, PART, PART, lanes)
        return head_at(yh if item == OWN_A else oyh, zz, cc, 0, PART, lanes)

    def lanes_of(step, dr):
        return None if step < 4 else (0 if dr == 0 else 1)

    def z_send(item, step, dr, src=None):
        zz = zdev(-DIRS[dr] * (step - 1))
        there = item_at(item, zz, c, lanes_of(step, dr))
        send(remote(
            there if src is None else src, there,
            zs.at[dr, step - 1, item], zr.at[dr, step - 1, item], z=zdev(DIRS[dr]),
        ))

    def z_wait(item, step, dr):
        here = item_at(item, zdev(-DIRS[dr] * step), c, lanes_of(step, dr))
        remote(
            here, here, zs.at[dr, step - 1, item], zr.at[dr, step - 1, item], z=zdev(DIRS[dr])
        ).wait_recv()
        return here

    def c_send(index, ref, src=None):
        send(remote(ref if src is None else src, ref, cs.at[index], cr.at[index], c=oc))

    def c_wait(index, ref):
        remote(ref, ref, cs.at[index], cr.at[index], c=oc).wait_recv()

    def c_index(item, step, dr):
        return 1 + (dr * 4 + step - 1) * 3 + item

    def y_send(index, ref, src=None):
        send(remote(ref if src is None else src, ref, ys.at[index], yr.at[index], yh=oyh))

    def y_wait(index, ref):
        remote(ref, ref, ys.at[index], yr.at[index], yh=oyh).wait_recv()

    def y_index(step, dr):
        return 2 + dr * 4 + step - 1

    def peer_b(step, dr, cc):
        return head_at(oyh, zdev(-DIRS[dr] * step), cc, PART, PART, lanes_of(step, dr))

    def hid_at(v, half=None):
        if half is None:
            return X.at[pl.ds(pl.multiple_of(v * HOME, HOME), HOME), :]
        return X.at[pl.ds(pl.multiple_of(v * HOME + half * 32, 32), 32), :]

    sum_copy(0, 0).start()
    for n, (dx, dy) in enumerate(vocab_peers):
        send(remote(tgt_ref, A.at[me], as_.at[n], ar.at[n], **vpeer(dx, dy)))
    own_a, own_b = head_ref.at[pl.ds(0, PART), :], head_ref.at[pl.ds(PART, PART), :]
    y_send(0, head_at(yh, z, c, 0, PART), own_a)
    for item, own in ((B, own_b), (OWN_A, own_a)):
        for dr in range(2):
            z_send(item, 1, dr, own)
    for dr in range(2):
        send(remote(hid_ref, hid_at(me), hs.at[1 + dr], hr.at[1 + dr], x=xdev(DIRS[dr])))
    y_send(1, head_at(yh, z, c, PART, PART), own_b)
    send(remote(hid_ref, hid_at(me), hs.at[0], hr.at[0], yl=oyl))
    c_send(0, head_at(yh, z, c, 0, HEAD_ROWS), head_ref)

    def pass_on(items, step):
        for item in items:
            for dr in range(2):
                here = z_wait(item, step, dr)
                if step < 4:
                    z_send(item, step + 1, dr)
                if item == B:
                    y_send(y_index(step, dr), here)
                c_send(c_index(item, step, dr), here)

    def take_y(step):
        for dr in range(2):
            ref = peer_b(step, dr, c)
            y_wait(y_index(step, dr), ref)
            c_send(27 + dr * 4 + step - 1, ref)

    def take_c(step, own):
        for dr in range(2):
            for item in (B, OWN_A) if own else (PEER_A,):
                c_wait(
                    c_index(item, step, dr),
                    item_at(item, zdev(-DIRS[dr] * step), oc, lanes_of(step, dr)),
                )
            if not own:
                c_wait(27 + dr * 4 + step - 1, peer_b(step, dr, oc))

    def hid_pass(kind):
        for dr in range(2):
            v = xdev(-DIRS[dr]) * 2 + (yl if kind == 0 else oyl)
            ref = hid_at(v)
            n = 1 + 2 * kind + dr
            remote(ref, ref, hs.at[n], hr.at[n], x=xdev(DIRS[dr])).wait_recv()
            half = hid_at(v, dr)
            n = 5 + 2 * kind + dr
            send(remote(half, half, hs.at[n], hr.at[n], x=xdev(DIRS[dr])))

    def hid_far(kind):
        for dr in range(2):
            half = hid_at(xdev(2) * 2 + (yl if kind == 0 else oyl), dr)
            n = 5 + 2 * kind + dr
            remote(half, half, hs.at[n], hr.at[n], x=xdev(DIRS[dr])).wait_recv()

    def multiply(quad, ring, fresh=False):
        start = pl.multiple_of(ring * 1536 + quad * QUAD, 256)

        def tile(n, carry):
            at = pl.ds(pl.multiple_of(n * 512, 512), 512)
            part = jnp.dot(
                X[:, pl.ds(start, QUAD)], H[pl.ds(start, QUAD), at],
                preferred_element_type=jnp.float32,
            )
            if fresh:
                L[:, at] = part
            else:
                L[:, at] += part
            return carry

        lax.fori_loop(0, LEVELS // 512, tile, 0)

    near = lax.div(z, 4)
    far = 1 - near

    pass_on((B,), 1)
    ref = head_at(oyh, z, c, 0, PART)
    y_wait(0, ref)
    for dr in range(2):
        z_send(PEER_A, 1, dr)
    c_send(25, ref)
    pass_on((OWN_A,), 1)
    sum_stage(0, 1)
    hid_pass(0)
    ref = head_at(oyh, z, c, PART, PART)
    y_wait(1, ref)
    c_send(26, ref)
    pass_on((B,), 2)
    hid_peer = hid_at(x * 2 + oyl)
    remote(hid_peer, hid_peer, hs.at[0], hr.at[0], yl=oyl).wait_recv()
    for dr in range(2):
        send(remote(hid_peer, hid_peer, hs.at[3 + dr], hr.at[3 + dr], x=xdev(DIRS[dr])))
    pass_on((PEER_A,), 1)
    pass_on((OWN_A,), 2)
    take_y(1)
    sum_stage(0, 2)
    pass_on((B,), 3)
    hid_pass(1)
    pass_on((PEER_A,), 2)
    pass_on((OWN_A,), 3)
    take_y(2)
    pass_on((B,), 4)
    for copy in own_copies:
        copy.wait()
    for n, (dx, dy) in enumerate(vocab_peers):
        there = A.at[vindex(dx, dy)]
        remote(tgt_ref, there, as_.at[n], ar.at[n], **vpeer(dx, dy)).wait_recv()
    c_wait(0, head_at(yh, z, oc, 0, HEAD_ROWS))
    hid_far(0)
    hid_far(1)
    for step in (1, 2, 3):
        take_c(step, True)
    multiply(near, yh, True)
    pass_on((PEER_A,), 3)
    pass_on((OWN_A,), 4)
    take_y(3)
    take_c(4, True)
    multiply(far, yh)
    pass_on((PEER_A,), 4)
    c_wait(25, head_at(oyh, z, oc, 0, PART))
    c_wait(26, head_at(oyh, z, oc, PART, PART))
    for step in (1, 2, 3):
        take_c(step, False)
    multiply(near, oyh)
    take_y(4)
    count_tile = sum_stage(0, 3)
    take_c(4, False)
    multiply(far, oyh)

    base = me * LEVELS
    lane = lax.broadcasted_iota(jnp.int32, (HOME, 128), 1)
    eye = lane == lax.broadcasted_iota(jnp.int32, (HOME, 128), 0)
    level = lax.broadcasted_iota(jnp.int32, (HOME, LEVELS), 1)

    def to_row(column):
        return jnp.sum(jnp.where(eye, column, 0.0), axis=0, keepdims=True)

    def to_column(row):
        return jnp.sum(jnp.where(eye, row, 0.0), axis=1, keepdims=True)

    def target_of(v):
        row = A[v].astype(jnp.float32)
        return jnp.sum(jnp.where(eye[:, :HOME], row, 0.0), axis=1, keepdims=True).astype(jnp.int32) - base

    def rows_of(v):
        return pl.ds(pl.multiple_of(v * HOME, HOME), HOME)

    def statistics(v, carry):
        logits = L[rows_of(v), :]
        top = jnp.max(logits, axis=1, keepdims=True)
        total = jnp.sum(jnp.exp(logits - top), axis=1, keepdims=True)
        hit = jnp.sum(jnp.where(level == target_of(v), logits, 0.0), axis=1, keepdims=True)
        for n, column in enumerate((top, total, hit)):
            ST[me, n, pl.ds(v, 1), :] = to_row(column)
        return carry

    lax.fori_loop(0, 8, statistics, 0)
    for n, (dx, dy) in enumerate(vocab_peers):
        send(remote(ST.at[me], ST.at[me], ts.at[n], tr.at[n], **vpeer(dx, dy)))
    for n, (dx, dy) in enumerate(vocab_peers):
        there = ST.at[vindex(dx, dy)]
        remote(ST.at[me], there, ts.at[n], tr.at[n], **vpeer(dx, dy)).wait_recv()

    top = ST[0, 0]
    for v in range(1, 8):
        top = jnp.maximum(top, ST[v, 0])
    total = jnp.zeros((8, 128), jnp.float32)
    hit = jnp.zeros((8, 128), jnp.float32)
    for v in range(8):
        total = total + ST[v, 1] * jnp.exp(ST[v, 0] - top)
        hit = hit + ST[v, 2]
    log_total = top + jnp.log(total)
    LS[...] = log_total

    length = len_ref[0]
    lane8 = lax.broadcasted_iota(jnp.int32, (8, 128), 1)
    place = lax.broadcasted_iota(jnp.int32, (8, 128), 0) * HOME + lane8
    counted = (lane8 < HOME) & (place < length)
    row_loss = jnp.where(counted, log_total - hit, 0.0)
    clip_loss = jnp.sum(jnp.sum(row_loss, axis=1, keepdims=True), axis=0, keepdims=True)
    SB[1, 0] = jnp.broadcast_to(clip_loss, (8, 128))
    count = count_tile[0:1, 0:1]

    def gradient(v, carry):
        place = v * HOME + lax.broadcasted_iota(jnp.int32, (HOME, 1), 0)
        weight = jnp.where(place < length, 1.0, 0.0) / count
        share = jnp.exp(L[rows_of(v), :] - to_column(LS[pl.ds(v, 1), :]))
        share = share - jnp.where(level == target_of(v), 1.0, 0.0)
        G[rows_of(v), :] = (weight * share).astype(jnp.bfloat16)
        return carry

    lax.fori_loop(0, 8, gradient, 0)
    sum_copy(1, 0).start()

    def f32(value):
        return value.astype(jnp.float32)

    def turn(j):
        return 1 if j % 2 else -1

    def compute(j):
        rows = pl.ds(j * CHUNK, CHUNK)
        product = lax.dot_general(
            G[...], H[rows, :], (((1,), (1,)), ((), ())), preferred_element_type=jnp.float32
        )
        PT[j] = product.astype(jnp.bfloat16).reshape(4, 2, HOME, CHUNK)

    def write(j, value):
        grad_ref[:, j * CHUNK : (j + 1) * CHUNK] = value.astype(jnp.bfloat16)

    def y_copy(j, kind):
        d = turn(j)
        if kind == 0:
            return remote(PT.at[j, :, oyl], YF.at[j], ws.at[0, j], wr.at[0, j], yl=oyl)
        if kind == 1:
            return remote(SA.at[j, 0], YR1.at[j], ws.at[1, j], wr.at[1, j], x=xdev(d))
        if kind == 2:
            return remote(SA.at[j, 1], YR2.at[j], ws.at[2, j], wr.at[2, j], x=xdev(-d))
        return remote(YS2.at[j], YR3.at[j], ws.at[3, j], wr.at[3, j], x=xdev(d))

    def y_sum(j, xx):
        return f32(PT[j, xx, yl]) + f32(YF[j, xx])

    def y_first(j):
        y_copy(j, 0).wait_recv()
        SA[j, 0] = y_sum(j, xdev(2)).astype(jnp.bfloat16)
        SA[j, 1] = y_sum(j, xdev(-turn(j))).astype(jnp.bfloat16)
        y_copy(j, 1).start()
        y_copy(j, 2).start()

    def y_second(j):
        y_copy(j, 1).wait_recv()
        YS2[j] = (y_sum(j, xdev(turn(j))) + f32(YR1[j])).astype(jnp.bfloat16)
        y_copy(j, 3).start()

    def y_last(j):
        y_copy(j, 2).wait_recv()
        y_copy(j, 3).wait_recv()
        write(j, y_sum(j, x) + f32(YR2[j]) + f32(YR3[j]))

    def x_copy(j, kind):
        d, k = turn(j), j - YC
        if kind == 0:
            return remote(PT.at[j, xdev(2)], XR1.at[k], xs.at[0, k], xr.at[0, k], x=xdev(d))
        if kind == 1:
            return remote(PT.at[j, xdev(-d)], XR2.at[k], xs.at[1, k], xr.at[1, k], x=xdev(-d))
        if kind == 2:
            return remote(XS2.at[k], XR3.at[k], xs.at[2, k], xr.at[2, k], x=xdev(d))
        return remote(SY.at[k], YR.at[k], xs.at[3, k], xr.at[3, k], yl=oyl)

    def x_first(j):
        x_copy(j, 0).start()
        x_copy(j, 1).start()

    def x_second(j):
        k = j - YC
        x_copy(j, 0).wait_recv()
        XS2[k] = (f32(PT[j, xdev(turn(j))]) + f32(XR1[k])).astype(jnp.bfloat16)
        x_copy(j, 2).start()

    def x_sum(j, which):
        k = j - YC
        return f32(PT[j, x, which]) + f32(XR2[k, which]) + f32(XR3[k, which])

    def x_third(j):
        k = j - YC
        x_copy(j, 1).wait_recv()
        x_copy(j, 2).wait_recv()
        SY[k] = x_sum(j, oyl).astype(jnp.bfloat16)
        x_copy(j, 3).start()

    def x_last(j):
        x_copy(j, 3).wait_recv()
        write(j, x_sum(j, yl) + f32(YR[j - YC]))

    compute(0)
    y_copy(0, 0).start()
    compute(1)
    y_copy(1, 0).start()
    compute(2)
    x_first(2)
    compute(3)
    x_first(3)
    sum_stage(1, 1)
    compute(4)
    compute(5)
    x_second(2)
    y_first(0)
    x_first(4)
    x_second(3)
    sum_stage(1, 2)
    y_second(0)
    x_first(5)
    y_first(1)
    x_second(4)
    x_third(2)
    x_third(3)
    y_second(1)
    x_second(5)
    y_last(0)
    x_third(4)
    x_last(2)
    x_last(3)
    x_third(5)
    y_last(1)
    x_last(4)

    loss = sum_stage(1, 3) / count_tile
    loss_ref[0, 0] = loss[0, 0]
    x_last(5)
    for copy in sent:
        copy.wait_send()
    for kind in range(4):
        for j in range(YC):
            y_copy(j, kind).wait_send()
        for j in range(YC, CHUNKS):
            x_copy(j, kind).wait_send()


def local(hidden, targets, lengths, head):
    bf16, f32, i32 = jnp.bfloat16, jnp.float32, jnp.int32
    vmem = pl.BlockSpec(memory_space=pltpu.VMEM)
    smem = pl.BlockSpec(memory_space=pltpu.SMEM)
    dma = pltpu.SemaphoreType.DMA
    grad, loss = pl.pallas_call(
        kernel,
        out_shape=(
            jax.ShapeDtypeStruct((HOME, WIDTH), bf16),
            jax.ShapeDtypeStruct((1, 1), f32),
        ),
        in_specs=[vmem, vmem, smem, vmem],
        out_specs=(vmem, smem),
        scratch_shapes=[
            pltpu.VMEM((WIDTH, LEVELS), bf16),
            pltpu.VMEM((ROWS, WIDTH), bf16),
            pltpu.VMEM((8, 1, HOME), i32),
            pltpu.VMEM((ROWS, LEVELS), f32),
            pltpu.VMEM((ROWS, LEVELS), bf16),
            pltpu.VMEM((CHUNKS, 4, 2, HOME, CHUNK), bf16),
            pltpu.VMEM((XC, 2, HOME, CHUNK), bf16),
            pltpu.VMEM((XC, 2, HOME, CHUNK), bf16),
            pltpu.VMEM((XC, 2, HOME, CHUNK), bf16),
            pltpu.VMEM((XC, 2, HOME, CHUNK), bf16),
            pltpu.VMEM((XC, HOME, CHUNK), bf16),
            pltpu.VMEM((XC, HOME, CHUNK), bf16),
            pltpu.VMEM((YC, 4, HOME, CHUNK), bf16),
            pltpu.VMEM((YC, 2, HOME, CHUNK), bf16),
            pltpu.VMEM((YC, HOME, CHUNK), bf16),
            pltpu.VMEM((YC, HOME, CHUNK), bf16),
            pltpu.VMEM((YC, HOME, CHUNK), bf16),
            pltpu.VMEM((YC, HOME, CHUNK), bf16),
            pltpu.VMEM((8, 3, 8, 128), f32),
            pltpu.VMEM((8, 128), f32),
            pltpu.VMEM((2, 12, 8, 128), f32),
            dma((2, 4, 3)), dma((2, 4, 3)),
            dma((10,)), dma((10,)),
            dma((35,)), dma((35,)),
            dma((9,)), dma((9,)),
            dma((7,)), dma((7,)),
            dma((7,)), dma((7,)),
            dma((2, 9)), dma((2, 9)),
            dma((4, XC)), dma((4, XC)),
            dma((4, YC)), dma((4, YC)),
            dma((3,)),
        ],
        compiler_params=pltpu.CompilerParams(
            collective_id=0, has_side_effects=True, vmem_limit_bytes=58 * 2**20
        ),
    )(hidden, targets.reshape(1, HOME), lengths, head)
    return grad, loss.reshape(())


def solution(mesh):
    torus = Mesh(mesh.devices.reshape(SIZES), AXES)
    return jax.shard_map(
        local,
        mesh=torus,
        in_specs=(P(DP + VOCAB, None), P(DP + VOCAB), P(DP), P(DP, VOCAB)),
        out_specs=(P(DP + VOCAB, None), P()),
        check_vma=False,
    )
```

```python
import jax
import jax.numpy as jnp
from jax import lax
from jax.experimental import pallas as pl
from jax.experimental.pallas import tpu as pltpu
from jax.sharding import Mesh
from jax.sharding import PartitionSpec as P

AXES = ("yh", "z", "c", "x", "yl")
SIZES = (2, 8, 2, 4, 2)
DP = ("yh", "z", "c")
VOCAB = ("x", "yl")
MESH = pl.DeviceIdType.MESH

WIDTH = 3072
LEVELS = 2048
HOME = 64
ROWS = 512
HEAD_ROWS = 96
PART = 48
HALF = LEVELS // 2
CHUNKS = 6
CHUNK = WIDTH // CHUNKS
QUAD = 768
XC, YC = 4, 2


def kernel(
    hid_ref, tgt_ref, len_ref, head_ref, grad_ref, loss_ref,
    H, X, A, L, G, PT, XR1, XR2, XR3, XS2, SY, YR, YF, SA, YR1, YR2, YR3, YS2, ST, LS, SB,
    zs, zr, ys, yr, cs, cr, hs, hr, as_, ar, ts, tr, ss, sr, xs, xr, ws, wr, ls,
):
    yh, z, c, x, yl = (lax.axis_index(name) for name in AXES)
    oyh, oc, oyl = 1 - yh, 1 - c, 1 - yl
    me = x * 2 + yl

    def remote(src, dst, send, recv, **device):
        return pltpu.make_async_remote_copy(
            src_ref=src, dst_ref=dst, send_sem=send, recv_sem=recv,
            device_id=device, device_id_type=MESH,
        )

    def zdev(d):
        return lax.rem(z + d + 8, 8)

    def xdev(d):
        return lax.rem(x + d + 4, 4)

    vocab_peers = [(dx, dy) for dx in range(4) for dy in range(2) if dx or dy]

    def vpeer(dx, dy):
        return dict(x=xdev(dx), yl=lax.rem(yl + dy, 2))

    def vindex(dx, dy):
        return xdev(-dx) * 2 + lax.rem(yl + dy, 2)

    barrier = pltpu.get_barrier_semaphore()
    peers = [dict(c=oc), dict(yh=oyh)]
    peers += [dict(z=zdev(d)) for d in range(1, 8)]
    peers += [vpeer(dx, dy) for dx, dy in vocab_peers]
    for device in peers:
        pl.semaphore_signal(barrier, 1, device_id=device, device_id_type=MESH)

    def row0(ring, zz, cc):
        return ring * 1536 + zz * 192 + cc * 96

    def head_at(ring, zz, cc, start, size, lanes=None):
        rows = pl.ds(pl.multiple_of(row0(ring, zz, cc) + start, 16), size)
        if lanes is None:
            return H.at[rows, :]
        return H.at[rows, pl.ds(lanes * HALF, HALF)]

    own_copies = [
        pltpu.make_async_copy(head_ref, head_at(yh, z, c, 0, HEAD_ROWS), ls.at[0]),
        pltpu.make_async_copy(hid_ref, X.at[pl.ds(pl.multiple_of(me * HOME, HOME), HOME), :], ls.at[1]),
        pltpu.make_async_copy(tgt_ref, A.at[me], ls.at[2]),
    ]
    for copy in own_copies:
        copy.start()
    SB[0, 0] = jnp.full((8, 128), len_ref[0], jnp.int32).astype(jnp.float32)
    pl.semaphore_wait(barrier, len(peers))

    sent = []

    def send(copy):
        copy.start()
        sent.append(copy)

    def sum_copy(k, stage, d=0):
        if stage == 0:
            return remote(SB.at[k, 0], SB.at[k, 1], ss.at[k, 0], sr.at[k, 0], c=oc)
        if stage == 1:
            return remote(SB.at[k, 2], SB.at[k, 3], ss.at[k, 1], sr.at[k, 1], yh=oyh)
        return remote(
            SB.at[k, 4 + z], SB.at[k, 4 + z], ss.at[k, 1 + d], sr.at[k, 1 + d], z=zdev(d)
        )

    def sum_stage(k, stage):
        if stage == 1:
            sum_copy(k, 0).wait_recv()
            SB[k, 2] = SB[k, 0] + SB[k, 1]
            sum_copy(k, 1).start()
        elif stage == 2:
            sum_copy(k, 1).wait_recv()
            SB[k, 4 + z] = SB[k, 2] + SB[k, 3]
            for d in range(1, 8):
                sum_copy(k, 2, d).start()
        elif stage == 3:
            for d in range(1, 8):
                remote(
                    SB.at[k, 4 + z], SB.at[k, 4 + zdev(-d)], ss.at[k, 1 + d], sr.at[k, 1 + d], z=zdev(d)
                ).wait_recv()
            total = SB[k, 4]
            for n in range(1, 8):
                total = total + SB[k, 4 + n]
            for stage_ in range(2):
                sum_copy(k, stage_).wait_send()
            for d in range(1, 8):
                sum_copy(k, 2, d).wait_send()
            return total

    DIRS = (1, -1)
    B, OWN_A, PEER_A = 0, 1, 2

    def item_at(item, zz, cc, lanes=None):
        if item == B:
            return head_at(yh, zz, cc, PART, PART, lanes)
        return head_at(yh if item == OWN_A else oyh, zz, cc, 0, PART, lanes)

    def lanes_of(step, dr):
        return None if step < 4 else (0 if dr == 0 else 1)

    def z_send(item, step, dr, src=None):
        zz = zdev(-DIRS[dr] * (step - 1))
        there = item_at(item, zz, c, lanes_of(step, dr))
        send(remote(
            there if src is None else src, there,
            zs.at[dr, step - 1, item], zr.at[dr, step - 1, item], z=zdev(DIRS[dr]),
        ))

    def z_wait(item, step, dr):
        here = item_at(item, zdev(-DIRS[dr] * step), c, lanes_of(step, dr))
        remote(
            here, here, zs.at[dr, step - 1, item], zr.at[dr, step - 1, item], z=zdev(DIRS[dr])
        ).wait_recv()
        return here

    def c_send(index, ref, src=None):
        send(remote(ref if src is None else src, ref, cs.at[index], cr.at[index], c=oc))

    def c_wait(index, ref):
        remote(ref, ref, cs.at[index], cr.at[index], c=oc).wait_recv()

    def c_index(item, step, dr):
        return 1 + (dr * 4 + step - 1) * 3 + item

    def y_send(index, ref, src=None):
        send(remote(ref if src is None else src, ref, ys.at[index], yr.at[index], yh=oyh))

    def y_wait(index, ref):
        remote(ref, ref, ys.at[index], yr.at[index], yh=oyh).wait_recv()

    def y_index(step, dr):
        return 2 + dr * 4 + step - 1

    def peer_b(step, dr, cc):
        return head_at(oyh, zdev(-DIRS[dr] * step), cc, PART, PART, lanes_of(step, dr))

    def hid_at(v, half=None):
        if half is None:
            return X.at[pl.ds(pl.multiple_of(v * HOME, HOME), HOME), :]
        return X.at[pl.ds(pl.multiple_of(v * HOME + half * 32, 32), 32), :]

    sum_copy(0, 0).start()
    for n, (dx, dy) in enumerate(vocab_peers):
        send(remote(tgt_ref, A.at[me], as_.at[n], ar.at[n], **vpeer(dx, dy)))
    own_a, own_b = head_ref.at[pl.ds(0, PART), :], head_ref.at[pl.ds(PART, PART), :]
    y_send(0, head_at(yh, z, c, 0, PART), own_a)
    for item, own in ((B, own_b), (OWN_A, own_a)):
        for dr in range(2):
            z_send(item, 1, dr, own)
    for dr in range(2):
        send(remote(hid_ref, hid_at(me), hs.at[1 + dr], hr.at[1 + dr], x=xdev(DIRS[dr])))
    y_send(1, head_at(yh, z, c, PART, PART), own_b)
    send(remote(hid_ref, hid_at(me), hs.at[0], hr.at[0], yl=oyl))
    c_send(0, head_at(yh, z, c, 0, HEAD_ROWS), head_ref)

    def pass_on(items, step):
        for item in items:
            for dr in range(2):
                here = z_wait(item, step, dr)
                if step < 4:
                    z_send(item, step + 1, dr)
                if item == B:
                    y_send(y_index(step, dr), here)
                c_send(c_index(item, step, dr), here)

    def take_y(step):
        for dr in range(2):
            ref = peer_b(step, dr, c)
            y_wait(y_index(step, dr), ref)
            c_send(27 + dr * 4 + step - 1, ref)

    def take_c(step, own):
        for dr in range(2):
            for item in (B, OWN_A) if own else (PEER_A,):
                c_wait(
                    c_index(item, step, dr),
                    item_at(item, zdev(-DIRS[dr] * step), oc, lanes_of(step, dr)),
                )
            if not own:
                c_wait(27 + dr * 4 + step - 1, peer_b(step, dr, oc))

    def hid_pass(kind):
        for dr in range(2):
            v = xdev(-DIRS[dr]) * 2 + (yl if kind == 0 else oyl)
            ref = hid_at(v)
            n = 1 + 2 * kind + dr
            remote(ref, ref, hs.at[n], hr.at[n], x=xdev(DIRS[dr])).wait_recv()
            half = hid_at(v, dr)
            n = 5 + 2 * kind + dr
            send(remote(half, half, hs.at[n], hr.at[n], x=xdev(DIRS[dr])))

    def hid_far(kind):
        for dr in range(2):
            half = hid_at(xdev(2) * 2 + (yl if kind == 0 else oyl), dr)
            n = 5 + 2 * kind + dr
            remote(half, half, hs.at[n], hr.at[n], x=xdev(DIRS[dr])).wait_recv()

    def multiply(quad, ring, fresh=False):
        start = pl.multiple_of(ring * 1536 + quad * QUAD, 256)

        def tile(n, carry):
            at = pl.ds(pl.multiple_of(n * 512, 512), 512)
            part = jnp.dot(
                X[:, pl.ds(start, QUAD)], H[pl.ds(start, QUAD), at],
                preferred_element_type=jnp.float32,
            )
            if fresh:
                L[:, at] = part
            else:
                L[:, at] += part
            return carry

        lax.fori_loop(0, LEVELS // 512, tile, 0)

    near = lax.div(z, 4)
    far = 1 - near

    pass_on((B,), 1)
    ref = head_at(oyh, z, c, 0, PART)
    y_wait(0, ref)
    for dr in range(2):
        z_send(PEER_A, 1, dr)
    c_send(25, ref)
    pass_on((OWN_A,), 1)
    sum_stage(0, 1)
    hid_pass(0)
    ref = head_at(oyh, z, c, PART, PART)
    y_wait(1, ref)
    c_send(26, ref)
    pass_on((B,), 2)
    hid_peer = hid_at(x * 2 + oyl)
    remote(hid_peer, hid_peer, hs.at[0], hr.at[0], yl=oyl).wait_recv()
    for dr in range(2):
        send(remote(hid_peer, hid_peer, hs.at[3 + dr], hr.at[3 + dr], x=xdev(DIRS[dr])))
    pass_on((PEER_A,), 1)
    pass_on((OWN_A,), 2)
    take_y(1)
    sum_stage(0, 2)
    pass_on((B,), 3)
    hid_pass(1)
    pass_on((PEER_A,), 2)
    pass_on((OWN_A,), 3)
    take_y(2)
    pass_on((B,), 4)
    for copy in own_copies:
        copy.wait()
    for n, (dx, dy) in enumerate(vocab_peers):
        there = A.at[vindex(dx, dy)]
        remote(tgt_ref, there, as_.at[n], ar.at[n], **vpeer(dx, dy)).wait_recv()
    c_wait(0, head_at(yh, z, oc, 0, HEAD_ROWS))
    hid_far(0)
    hid_far(1)
    for step in (1, 2, 3):
        take_c(step, True)
    multiply(near, yh, True)
    pass_on((PEER_A,), 3)
    pass_on((OWN_A,), 4)
    take_y(3)
    take_c(4, True)
    multiply(far, yh)
    pass_on((PEER_A,), 4)
    c_wait(25, head_at(oyh, z, oc, 0, PART))
    c_wait(26, head_at(oyh, z, oc, PART, PART))
    for step in (1, 2, 3):
        take_c(step, False)
    multiply(near, oyh)
    take_y(4)
    count_tile = sum_stage(0, 3)
    take_c(4, False)
    multiply(far, oyh)

    base = me * LEVELS
    lane = lax.broadcasted_iota(jnp.int32, (HOME, 128), 1)
    eye = lane == lax.broadcasted_iota(jnp.int32, (HOME, 128), 0)
    level = lax.broadcasted_iota(jnp.int32, (HOME, LEVELS), 1)

    def to_row(column):
        return jnp.sum(jnp.where(eye, column, 0.0), axis=0, keepdims=True)

    def to_column(row):
        return jnp.sum(jnp.where(eye, row, 0.0), axis=1, keepdims=True)

    def target_of(v):
        row = A[v].astype(jnp.float32)
        return jnp.sum(jnp.where(eye[:, :HOME], row, 0.0), axis=1, keepdims=True).astype(jnp.int32) - base

    def rows_of(v):
        return pl.ds(pl.multiple_of(v * HOME, HOME), HOME)

    def statistics(v, carry):
        logits = L[rows_of(v), :]
        top = jnp.max(logits, axis=1, keepdims=True)
        total = jnp.sum(jnp.exp(logits - top), axis=1, keepdims=True)
        hit = jnp.sum(jnp.where(level == target_of(v), logits, 0.0), axis=1, keepdims=True)
        for n, column in enumerate((top, total, hit)):
            ST[me, n, pl.ds(v, 1), :] = to_row(column)
        return carry

    lax.fori_loop(0, 8, statistics, 0)
    for n, (dx, dy) in enumerate(vocab_peers):
        send(remote(ST.at[me], ST.at[me], ts.at[n], tr.at[n], **vpeer(dx, dy)))
    for n, (dx, dy) in enumerate(vocab_peers):
        there = ST.at[vindex(dx, dy)]
        remote(ST.at[me], there, ts.at[n], tr.at[n], **vpeer(dx, dy)).wait_recv()

    top = ST[0, 0]
    for v in range(1, 8):
        top = jnp.maximum(top, ST[v, 0])
    total = jnp.zeros((8, 128), jnp.float32)
    hit = jnp.zeros((8, 128), jnp.float32)
    for v in range(8):
        total = total + ST[v, 1] * jnp.exp(ST[v, 0] - top)
        hit = hit + ST[v, 2]
    log_total = top + jnp.log(total)
    LS[...] = log_total

    length = len_ref[0]
    lane8 = lax.broadcasted_iota(jnp.int32, (8, 128), 1)
    place = lax.broadcasted_iota(jnp.int32, (8, 128), 0) * HOME + lane8
    counted = (lane8 < HOME) & (place < length)
    row_loss = jnp.where(counted, log_total - hit, 0.0)
    clip_loss = jnp.sum(jnp.sum(row_loss, axis=1, keepdims=True), axis=0, keepdims=True)
    SB[1, 0] = jnp.broadcast_to(clip_loss, (8, 128))
    count = count_tile[0:1, 0:1]

    def gradient(v, carry):
        place = v * HOME + lax.broadcasted_iota(jnp.int32, (HOME, 1), 0)
        weight = jnp.where(place < length, 1.0, 0.0) / count
        share = jnp.exp(L[rows_of(v), :] - to_column(LS[pl.ds(v, 1), :]))
        share = share - jnp.where(level == target_of(v), 1.0, 0.0)
        G[rows_of(v), :] = (weight * share).astype(jnp.bfloat16)
        return carry

    lax.fori_loop(0, 8, gradient, 0)
    sum_copy(1, 0).start()

    def f32(value):
        return value.astype(jnp.float32)

    def turn(j):
        return 1 if j % 2 else -1

    def compute(j):
        rows = pl.ds(j * CHUNK, CHUNK)
        product = lax.dot_general(
            G[...], H[rows, :], (((1,), (1,)), ((), ())), preferred_element_type=jnp.float32
        )
        PT[j] = product.astype(jnp.bfloat16).reshape(4, 2, HOME, CHUNK)

    def write(j, value):
        grad_ref[:, j * CHUNK : (j + 1) * CHUNK] = value.astype(jnp.bfloat16)

    def y_copy(j, kind):
        d = turn(j)
        if kind == 0:
            return remote(PT.at[j, :, oyl], YF.at[j], ws.at[0, j], wr.at[0, j], yl=oyl)
        if kind == 1:
            return remote(SA.at[j, 0], YR1.at[j], ws.at[1, j], wr.at[1, j], x=xdev(d))
        if kind == 2:
            return remote(SA.at[j, 1], YR2.at[j], ws.at[2, j], wr.at[2, j], x=xdev(-d))
        return remote(YS2.at[j], YR3.at[j], ws.at[3, j], wr.at[3, j], x=xdev(d))

    def y_sum(j, xx):
        return f32(PT[j, xx, yl]) + f32(YF[j, xx])

    def y_first(j):
        y_copy(j, 0).wait_recv()
        SA[j, 0] = y_sum(j, xdev(2)).astype(jnp.bfloat16)
        SA[j, 1] = y_sum(j, xdev(-turn(j))).astype(jnp.bfloat16)
        y_copy(j, 1).start()
        y_copy(j, 2).start()

    def y_second(j):
        y_copy(j, 1).wait_recv()
        YS2[j] = (y_sum(j, xdev(turn(j))) + f32(YR1[j])).astype(jnp.bfloat16)
        y_copy(j, 3).start()

    def y_last(j):
        y_copy(j, 2).wait_recv()
        y_copy(j, 3).wait_recv()
        write(j, y_sum(j, x) + f32(YR2[j]) + f32(YR3[j]))

    def x_copy(j, kind):
        d, k = turn(j), j - YC
        if kind == 0:
            return remote(PT.at[j, xdev(2)], XR1.at[k], xs.at[0, k], xr.at[0, k], x=xdev(d))
        if kind == 1:
            return remote(PT.at[j, xdev(-d)], XR2.at[k], xs.at[1, k], xr.at[1, k], x=xdev(-d))
        if kind == 2:
            return remote(XS2.at[k], XR3.at[k], xs.at[2, k], xr.at[2, k], x=xdev(d))
        return remote(SY.at[k], YR.at[k], xs.at[3, k], xr.at[3, k], yl=oyl)

    def x_first(j):
        x_copy(j, 0).start()
        x_copy(j, 1).start()

    def x_second(j):
        k = j - YC
        x_copy(j, 0).wait_recv()
        XS2[k] = (f32(PT[j, xdev(turn(j))]) + f32(XR1[k])).astype(jnp.bfloat16)
        x_copy(j, 2).start()

    def x_sum(j, which):
        k = j - YC
        return f32(PT[j, x, which]) + f32(XR2[k, which]) + f32(XR3[k, which])

    def x_third(j):
        k = j - YC
        x_copy(j, 1).wait_recv()
        x_copy(j, 2).wait_recv()
        SY[k] = x_sum(j, oyl).astype(jnp.bfloat16)
        x_copy(j, 3).start()

    def x_last(j):
        x_copy(j, 3).wait_recv()
        write(j, x_sum(j, yl) + f32(YR[j - YC]))

    compute(5)
    x_first(5)
    compute(3)
    x_first(3)
    compute(2)
    x_first(2)
    compute(1)
    y_copy(1, 0).start()
    compute(4)
    x_first(4)
    x_second(3)
    x_second(5)
    sum_stage(1, 1)
    compute(0)
    y_copy(0, 0).start()
    x_second(2)
    x_second(4)
    y_first(1)
    x_third(2)
    x_third(3)
    sum_stage(1, 2)
    y_first(0)
    x_third(4)
    y_second(1)
    x_third(5)
    x_last(2)
    y_second(0)
    y_last(1)
    x_last(4)
    x_last(5)
    x_last(3)

    loss = sum_stage(1, 3) / count_tile
    loss_ref[0, 0] = loss[0, 0]
    y_last(0)
    for copy in sent:
        copy.wait_send()
    for kind in range(4):
        for j in range(YC):
            y_copy(j, kind).wait_send()
        for j in range(YC, CHUNKS):
            x_copy(j, kind).wait_send()


def local(hidden, targets, lengths, head):
    bf16, f32, i32 = jnp.bfloat16, jnp.float32, jnp.int32
    vmem = pl.BlockSpec(memory_space=pltpu.VMEM)
    smem = pl.BlockSpec(memory_space=pltpu.SMEM)
    dma = pltpu.SemaphoreType.DMA
    grad, loss = pl.pallas_call(
        kernel,
        out_shape=(
            jax.ShapeDtypeStruct((HOME, WIDTH), bf16),
            jax.ShapeDtypeStruct((1, 1), f32),
        ),
        in_specs=[vmem, vmem, smem, vmem],
        out_specs=(vmem, smem),
        scratch_shapes=[
            pltpu.VMEM((WIDTH, LEVELS), bf16),
            pltpu.VMEM((ROWS, WIDTH), bf16),
            pltpu.VMEM((8, 1, HOME), i32),
            pltpu.VMEM((ROWS, LEVELS), f32),
            pltpu.VMEM((ROWS, LEVELS), bf16),
            pltpu.VMEM((CHUNKS, 4, 2, HOME, CHUNK), bf16),
            pltpu.VMEM((XC, 2, HOME, CHUNK), bf16),
            pltpu.VMEM((XC, 2, HOME, CHUNK), bf16),
            pltpu.VMEM((XC, 2, HOME, CHUNK), bf16),
            pltpu.VMEM((XC, 2, HOME, CHUNK), bf16),
            pltpu.VMEM((XC, HOME, CHUNK), bf16),
            pltpu.VMEM((XC, HOME, CHUNK), bf16),
            pltpu.VMEM((YC, 4, HOME, CHUNK), bf16),
            pltpu.VMEM((YC, 2, HOME, CHUNK), bf16),
            pltpu.VMEM((YC, HOME, CHUNK), bf16),
            pltpu.VMEM((YC, HOME, CHUNK), bf16),
            pltpu.VMEM((YC, HOME, CHUNK), bf16),
            pltpu.VMEM((YC, HOME, CHUNK), bf16),
            pltpu.VMEM((8, 3, 8, 128), f32),
            pltpu.VMEM((8, 128), f32),
            pltpu.VMEM((2, 12, 8, 128), f32),
            dma((2, 4, 3)), dma((2, 4, 3)),
            dma((10,)), dma((10,)),
            dma((35,)), dma((35,)),
            dma((9,)), dma((9,)),
            dma((7,)), dma((7,)),
            dma((7,)), dma((7,)),
            dma((2, 9)), dma((2, 9)),
            dma((4, XC)), dma((4, XC)),
            dma((4, YC)), dma((4, YC)),
            dma((3,)),
        ],
        compiler_params=pltpu.CompilerParams(
            collective_id=0, has_side_effects=True, vmem_limit_bytes=58 * 2**20
        ),
    )(hidden, targets.reshape(1, HOME), lengths, head)
    return grad, loss.reshape(())


def solution(mesh):
    torus = Mesh(mesh.devices.reshape(SIZES), AXES)
    return jax.shard_map(
        local,
        mesh=torus,
        in_specs=(P(DP + VOCAB, None), P(DP + VOCAB), P(DP), P(DP, VOCAB)),
        out_specs=(P(DP + VOCAB, None), P()),
        check_vma=False,
    )
```

```python
import jax
import jax.numpy as jnp
from jax import lax
from jax.experimental import pallas as pl
from jax.experimental.pallas import tpu as pltpu
from jax.sharding import Mesh
from jax.sharding import PartitionSpec as P

AXES = ("yh", "z", "c", "x", "yl")
SIZES = (2, 8, 2, 4, 2)
DP = ("yh", "z", "c")
VOCAB = ("x", "yl")
MESH = pl.DeviceIdType.MESH

WIDTH = 3072
LEVELS = 2048
HOME = 64
ROWS = 512
HEAD_ROWS = 96
PART = 48
HALF = LEVELS // 2
SUB = 32
CHUNKS = 6
CHUNK = WIDTH // 3
QUAD = 768
XC, YC = 4, 2
HALF_OF = (1, 0, 1, 0, 1, 0)
COLUMN_OF = (2, 2, 0, 1, 1, 0)
TURN = (-1, 1, 1, -1, -1, 1)


def kernel(
    hid_ref, tgt_ref, len_ref, head_ref, grad_ref, loss_ref,
    H, X, A, L, G, PT, XR1, XR2, XR3, XS2, SY, YR, YF, SA, YR1, YR2, YR3, YS2, ST, HT, LS, SB,
    zs, zr, ys, yr, cs, cr, hs, hr, as_, ar, ts, tr, ss, sr, xs, xr, ws, wr, ls,
):
    yh, z, c, x, yl = (lax.axis_index(name) for name in AXES)
    oyh, oc, oyl = 1 - yh, 1 - c, 1 - yl
    me = x * 2 + yl

    def remote(src, dst, send, recv, **device):
        return pltpu.make_async_remote_copy(
            src_ref=src, dst_ref=dst, send_sem=send, recv_sem=recv,
            device_id=device, device_id_type=MESH,
        )

    def zdev(d):
        return lax.rem(z + d + 8, 8)

    def xdev(d):
        return lax.rem(x + d + 4, 4)

    vocab_peers = [(dx, dy) for dx in range(4) for dy in range(2) if dx or dy]

    def vpeer(dx, dy):
        return dict(x=xdev(dx), yl=lax.rem(yl + dy, 2))

    def vindex(dx, dy):
        return xdev(-dx) * 2 + lax.rem(yl + dy, 2)

    barrier = pltpu.get_barrier_semaphore()
    peers = [dict(c=oc), dict(yh=oyh)]
    peers += [dict(z=zdev(d)) for d in range(1, 8)]
    peers += [vpeer(dx, dy) for dx, dy in vocab_peers]
    for device in peers:
        pl.semaphore_signal(barrier, 1, device_id=device, device_id_type=MESH)

    def row0(ring, zz, cc):
        return ring * 1536 + zz * 192 + cc * 96

    def head_at(ring, zz, cc, start, size, lanes=None):
        rows = pl.ds(pl.multiple_of(row0(ring, zz, cc) + start, 16), size)
        if lanes is None:
            return H.at[rows, :]
        return H.at[rows, pl.ds(lanes * HALF, HALF)]

    own_copies = [
        pltpu.make_async_copy(head_ref, head_at(yh, z, c, 0, HEAD_ROWS), ls.at[0]),
        pltpu.make_async_copy(hid_ref, X.at[:, me], ls.at[1]),
        pltpu.make_async_copy(tgt_ref, A.at[me], ls.at[2]),
    ]
    for copy in own_copies:
        copy.start()
    SB[0, 0] = jnp.full((8, 128), len_ref[0], jnp.int32).astype(jnp.float32)
    pl.semaphore_wait(barrier, len(peers))

    sent = []

    def send(copy):
        copy.start()
        sent.append(copy)

    def sum_copy(k, stage, d=0):
        if stage == 0:
            return remote(SB.at[k, 0], SB.at[k, 1], ss.at[k, 0], sr.at[k, 0], c=oc)
        if stage == 1:
            return remote(SB.at[k, 2], SB.at[k, 3], ss.at[k, 1], sr.at[k, 1], yh=oyh)
        return remote(
            SB.at[k, 4 + z], SB.at[k, 4 + z], ss.at[k, 1 + d], sr.at[k, 1 + d], z=zdev(d)
        )

    def sum_stage(k, stage):
        if stage == 1:
            sum_copy(k, 0).wait_recv()
            SB[k, 2] = SB[k, 0] + SB[k, 1]
            sum_copy(k, 1).start()
        elif stage == 2:
            sum_copy(k, 1).wait_recv()
            SB[k, 4 + z] = SB[k, 2] + SB[k, 3]
            for d in range(1, 8):
                sum_copy(k, 2, d).start()
        elif stage == 3:
            for d in range(1, 8):
                remote(
                    SB.at[k, 4 + z], SB.at[k, 4 + zdev(-d)], ss.at[k, 1 + d], sr.at[k, 1 + d], z=zdev(d)
                ).wait_recv()
            total = SB[k, 4]
            for n in range(1, 8):
                total = total + SB[k, 4 + n]
            for stage_ in range(2):
                sum_copy(k, stage_).wait_send()
            for d in range(1, 8):
                sum_copy(k, 2, d).wait_send()
            return total

    DIRS = (1, -1)
    B, OWN_A, PEER_A = 0, 1, 2

    def item_at(item, zz, cc, lanes=None):
        if item == B:
            return head_at(yh, zz, cc, PART, PART, lanes)
        return head_at(yh if item == OWN_A else oyh, zz, cc, 0, PART, lanes)

    def lanes_of(step, dr):
        return None if step < 4 else (0 if dr == 0 else 1)

    def z_send(item, step, dr, src=None):
        zz = zdev(-DIRS[dr] * (step - 1))
        there = item_at(item, zz, c, lanes_of(step, dr))
        send(remote(
            there if src is None else src, there,
            zs.at[dr, step - 1, item], zr.at[dr, step - 1, item], z=zdev(DIRS[dr]),
        ))

    def z_wait(item, step, dr):
        here = item_at(item, zdev(-DIRS[dr] * step), c, lanes_of(step, dr))
        remote(
            here, here, zs.at[dr, step - 1, item], zr.at[dr, step - 1, item], z=zdev(DIRS[dr])
        ).wait_recv()
        return here

    def c_send(index, ref, src=None):
        send(remote(ref if src is None else src, ref, cs.at[index], cr.at[index], c=oc))

    def c_wait(index, ref):
        remote(ref, ref, cs.at[index], cr.at[index], c=oc).wait_recv()

    def c_index(item, step, dr):
        return 1 + (dr * 4 + step - 1) * 3 + item

    def y_send(index, ref, src=None):
        send(remote(ref if src is None else src, ref, ys.at[index], yr.at[index], yh=oyh))

    def y_wait(index, ref):
        remote(ref, ref, ys.at[index], yr.at[index], yh=oyh).wait_recv()

    def y_index(step, dr):
        return 2 + dr * 4 + step - 1

    def peer_b(step, dr, cc):
        return head_at(oyh, zdev(-DIRS[dr] * step), cc, PART, PART, lanes_of(step, dr))

    def hid_at(v, half=None):
        return X.at[:, v] if half is None else X.at[half, v]

    sum_copy(0, 0).start()
    for n, (dx, dy) in enumerate(vocab_peers):
        send(remote(tgt_ref, A.at[me], as_.at[n], ar.at[n], **vpeer(dx, dy)))
    own_a, own_b = head_ref.at[pl.ds(0, PART), :], head_ref.at[pl.ds(PART, PART), :]
    y_send(0, head_at(yh, z, c, 0, PART), own_a)
    for item, own in ((B, own_b), (OWN_A, own_a)):
        for dr in range(2):
            z_send(item, 1, dr, own)
    for dr in range(2):
        send(remote(hid_ref, hid_at(me), hs.at[1 + dr], hr.at[1 + dr], x=xdev(DIRS[dr])))
    y_send(1, head_at(yh, z, c, PART, PART), own_b)
    send(remote(hid_ref, hid_at(me), hs.at[0], hr.at[0], yl=oyl))
    c_send(0, head_at(yh, z, c, 0, HEAD_ROWS), head_ref)

    def pass_on(items, step):
        for item in items:
            for dr in range(2):
                here = z_wait(item, step, dr)
                if step < 4:
                    z_send(item, step + 1, dr)
                if item == B:
                    y_send(y_index(step, dr), here)
                c_send(c_index(item, step, dr), here)

    def take_y(step):
        for dr in range(2):
            ref = peer_b(step, dr, c)
            y_wait(y_index(step, dr), ref)
            c_send(27 + dr * 4 + step - 1, ref)

    def take_c(step, own):
        for dr in range(2):
            for item in (B, OWN_A) if own else (PEER_A,):
                c_wait(
                    c_index(item, step, dr),
                    item_at(item, zdev(-DIRS[dr] * step), oc, lanes_of(step, dr)),
                )
            if not own:
                c_wait(27 + dr * 4 + step - 1, peer_b(step, dr, oc))

    def hid_pass(kind):
        for dr in range(2):
            v = xdev(-DIRS[dr]) * 2 + (yl if kind == 0 else oyl)
            ref = hid_at(v)
            n = 1 + 2 * kind + dr
            remote(ref, ref, hs.at[n], hr.at[n], x=xdev(DIRS[dr])).wait_recv()
            half = hid_at(v, dr)
            n = 5 + 2 * kind + dr
            send(remote(half, half, hs.at[n], hr.at[n], x=xdev(DIRS[dr])))

    def hid_far(kind):
        for dr in range(2):
            half = hid_at(xdev(2) * 2 + (yl if kind == 0 else oyl), dr)
            n = 5 + 2 * kind + dr
            remote(half, half, hs.at[n], hr.at[n], x=xdev(DIRS[dr])).wait_recv()

    def multiply(quad, ring, fresh=False, half=None):
        start = pl.multiple_of(ring * 1536 + quad * QUAD, 256)
        halves = slice(0, 2) if half is None else slice(half, half + 1)
        rows = slice(halves.start * 256, halves.stop * 256)
        width = 512 if half is None else 1024

        def tile(n, carry):
            at = pl.ds(pl.multiple_of(n * width, width), width)
            part = jnp.dot(
                X[halves, :, :, pl.ds(start, QUAD)].reshape(-1, QUAD),
                H[pl.ds(start, QUAD), at],
                preferred_element_type=jnp.float32,
            )
            if fresh:
                L[rows, at] = part
            else:
                L[rows, at] += part
            return carry

        lax.fori_loop(0, LEVELS // width, tile, 0)

    near = lax.div(z, 4)
    far = 1 - near

    pass_on((B,), 1)
    ref = head_at(oyh, z, c, 0, PART)
    y_wait(0, ref)
    for dr in range(2):
        z_send(PEER_A, 1, dr)
    c_send(25, ref)
    pass_on((OWN_A,), 1)
    sum_stage(0, 1)
    hid_pass(0)
    ref = head_at(oyh, z, c, PART, PART)
    y_wait(1, ref)
    c_send(26, ref)
    pass_on((B,), 2)
    hid_peer = hid_at(x * 2 + oyl)
    remote(hid_peer, hid_peer, hs.at[0], hr.at[0], yl=oyl).wait_recv()
    for dr in range(2):
        send(remote(hid_peer, hid_peer, hs.at[3 + dr], hr.at[3 + dr], x=xdev(DIRS[dr])))
    pass_on((PEER_A,), 1)
    pass_on((OWN_A,), 2)
    take_y(1)
    sum_stage(0, 2)
    pass_on((B,), 3)
    hid_pass(1)
    pass_on((PEER_A,), 2)
    pass_on((OWN_A,), 3)
    take_y(2)
    pass_on((B,), 4)
    for copy in own_copies:
        copy.wait()
    for n, (dx, dy) in enumerate(vocab_peers):
        there = A.at[vindex(dx, dy)]
        remote(tgt_ref, there, as_.at[n], ar.at[n], **vpeer(dx, dy)).wait_recv()
    c_wait(0, head_at(yh, z, oc, 0, HEAD_ROWS))
    hid_far(0)
    hid_far(1)
    for step in (1, 2, 3):
        take_c(step, True)
    multiply(near, yh, True)
    pass_on((PEER_A,), 3)
    pass_on((OWN_A,), 4)
    take_y(3)
    take_c(4, True)
    multiply(far, yh)
    pass_on((PEER_A,), 4)
    c_wait(25, head_at(oyh, z, oc, 0, PART))
    c_wait(26, head_at(oyh, z, oc, PART, PART))
    for step in (1, 2, 3):
        take_c(step, False)
    multiply(near, oyh)
    take_y(4)
    count_tile = sum_stage(0, 3)
    take_c(4, False)

    base = me * LEVELS
    lane = lax.broadcasted_iota(jnp.int32, (SUB, 128), 1)
    eye = lane == lax.broadcasted_iota(jnp.int32, (SUB, 128), 0)
    level = lax.broadcasted_iota(jnp.int32, (SUB, LEVELS), 1)
    place64 = lax.broadcasted_iota(jnp.int32, (SUB, HOME), 1)

    def to_row(column):
        return jnp.sum(jnp.where(eye, column, 0.0), axis=0, keepdims=True)

    def to_column(row):
        return jnp.sum(jnp.where(eye, row, 0.0), axis=1, keepdims=True)

    def target_of(half, v):
        row = A[v].astype(jnp.float32)
        here = place64 == lax.broadcasted_iota(jnp.int32, (SUB, HOME), 0) + half * SUB
        column = jnp.sum(jnp.where(here, row, 0.0), axis=1, keepdims=True)
        return column.astype(jnp.int32) - base

    def rows_of(half, v):
        return pl.ds(pl.multiple_of(half * 256 + v * SUB, SUB), SUB)

    def stat_copy(half, n, who):
        ref = ST.at[half, who] if half < 2 else HT.at[who]
        mine = ST.at[half, me] if half < 2 else HT.at[me]
        return remote(mine, ref, ts.at[half, n], tr.at[half, n], **vpeer(*vocab_peers[n]))

    def stat_send(half):
        for n in range(7):
            send(stat_copy(half, n, me))

    def stat_wait(half):
        for n, (dx, dy) in enumerate(vocab_peers):
            stat_copy(half, n, vindex(dx, dy)).wait_recv()

    def statistics(half):
        def block(v, carry):
            logits = L[rows_of(half, v), :]
            top = jnp.max(logits, axis=1, keepdims=True)
            total = jnp.sum(jnp.exp(logits - top), axis=1, keepdims=True)
            ST[half, me, 0, pl.ds(v, 1), :] = to_row(top)
            ST[half, me, 1, pl.ds(v, 1), :] = to_row(total)
            return carry

        for v in range(8):
            block(v, 0)
        stat_send(half)

    for half in range(2):
        multiply(far, oyh, half=half)
        statistics(half)

    def hits(half):
        def block(v, carry):
            found = jnp.where(level == target_of(half, v), L[rows_of(half, v), :], 0.0)
            HT[me, half, pl.ds(v, 1), :] = to_row(jnp.sum(found, axis=1, keepdims=True))
            return carry

        for v in range(8):
            block(v, 0)

    hits(0)
    hits(1)
    stat_send(2)

    length = len_ref[0]
    count = count_tile[0:1, 0:1]

    def gradient(half):
        stat_wait(half)
        top = ST[half, 0, 0]
        for v in range(1, 8):
            top = jnp.maximum(top, ST[half, v, 0])
        total = jnp.zeros((8, 128), jnp.float32)
        for v in range(8):
            total = total + ST[half, v, 1] * jnp.exp(ST[half, v, 0] - top)
        LS[half] = top + jnp.log(total)

        def block(v, carry):
            place = v * HOME + half * SUB + lax.broadcasted_iota(jnp.int32, (SUB, 1), 0)
            weight = jnp.where(place < length, 1.0, 0.0) / count
            share = jnp.exp(L[rows_of(half, v), :] - to_column(LS[half, pl.ds(v, 1), :]))
            share = share - jnp.where(level == target_of(half, v), 1.0, 0.0)
            G[rows_of(half, v), :] = (weight * share).astype(jnp.bfloat16)
            return carry

        for v in range(8):
            block(v, 0)

    def loss_start():
        stat_wait(2)
        lane8 = lax.broadcasted_iota(jnp.int32, (8, 128), 1)
        block8 = lax.broadcasted_iota(jnp.int32, (8, 128), 0)
        row_loss = jnp.zeros((8, 128), jnp.float32)
        for half in range(2):
            hit = HT[0, half]
            for v in range(1, 8):
                hit = hit + HT[v, half]
            counted = (lane8 < SUB) & (block8 * HOME + half * SUB + lane8 < length)
            row_loss = row_loss + jnp.where(counted, LS[half] - hit, 0.0)
        clip_loss = jnp.sum(jnp.sum(row_loss, axis=1, keepdims=True), axis=0, keepdims=True)
        SB[1, 0] = jnp.broadcast_to(clip_loss, (8, 128))
        sum_copy(1, 0).start()

    gradient(0)

    def f32(value):
        return value.astype(jnp.float32)

    def turn(j):
        return TURN[j]

    def columns(j):
        return pl.ds(COLUMN_OF[j] * CHUNK, CHUNK)

    def compute(j):
        product = lax.dot_general(
            G[pl.ds(HALF_OF[j] * 256, 256), :], H[columns(j), :], (((1,), (1,)), ((), ())),
            preferred_element_type=jnp.float32,
        )
        PT[j] = product.astype(jnp.bfloat16).reshape(4, 2, SUB, CHUNK)

    def write(j, value):
        grad_ref[HALF_OF[j], :, columns(j)] = value.astype(jnp.bfloat16)

    def y_copy(j, kind):
        d = turn(j)
        if kind == 0:
            return remote(PT.at[j, :, oyl], YF.at[j], ws.at[0, j], wr.at[0, j], yl=oyl)
        if kind == 1:
            return remote(SA.at[j, 0], YR1.at[j], ws.at[1, j], wr.at[1, j], x=xdev(d))
        if kind == 2:
            return remote(SA.at[j, 1], YR2.at[j], ws.at[2, j], wr.at[2, j], x=xdev(-d))
        return remote(YS2.at[j], YR3.at[j], ws.at[3, j], wr.at[3, j], x=xdev(d))

    def y_sum(j, xx):
        return f32(PT[j, xx, yl]) + f32(YF[j, xx])

    def y_first(j):
        y_copy(j, 0).wait_recv()
        SA[j, 0] = y_sum(j, xdev(2)).astype(jnp.bfloat16)
        SA[j, 1] = y_sum(j, xdev(-turn(j))).astype(jnp.bfloat16)
        y_copy(j, 1).start()
        y_copy(j, 2).start()

    def y_second(j):
        y_copy(j, 1).wait_recv()
        YS2[j] = (y_sum(j, xdev(turn(j))) + f32(YR1[j])).astype(jnp.bfloat16)
        y_copy(j, 3).start()

    def y_last(j):
        y_copy(j, 2).wait_recv()
        y_copy(j, 3).wait_recv()
        write(j, y_sum(j, x) + f32(YR2[j]) + f32(YR3[j]))

    def x_copy(j, kind):
        d, k = turn(j), j - YC
        if kind == 0:
            return remote(PT.at[j, xdev(2)], XR1.at[k], xs.at[0, k], xr.at[0, k], x=xdev(d))
        if kind == 1:
            return remote(PT.at[j, xdev(-d)], XR2.at[k], xs.at[1, k], xr.at[1, k], x=xdev(-d))
        if kind == 2:
            return remote(XS2.at[k], XR3.at[k], xs.at[2, k], xr.at[2, k], x=xdev(d))
        return remote(SY.at[k], YR.at[k], xs.at[3, k], xr.at[3, k], yl=oyl)

    def x_first(j):
        x_copy(j, 0).start()
        x_copy(j, 1).start()

    def x_second(j):
        k = j - YC
        x_copy(j, 0).wait_recv()
        XS2[k] = (f32(PT[j, xdev(turn(j))]) + f32(XR1[k])).astype(jnp.bfloat16)
        x_copy(j, 2).start()

    def x_sum(j, which):
        k = j - YC
        return f32(PT[j, x, which]) + f32(XR2[k, which]) + f32(XR3[k, which])

    def x_third(j):
        k = j - YC
        x_copy(j, 1).wait_recv()
        x_copy(j, 2).wait_recv()
        SY[k] = x_sum(j, oyl).astype(jnp.bfloat16)
        x_copy(j, 3).start()

    def x_last(j):
        x_copy(j, 3).wait_recv()
        write(j, x_sum(j, yl) + f32(YR[j - YC]))

    compute(3)
    x_first(3)
    compute(5)
    x_first(5)
    compute(1)
    y_copy(1, 0).start()
    gradient(1)
    compute(4)
    x_first(4)
    compute(0)
    y_copy(0, 0).start()
    compute(2)
    x_first(2)
    loss_start()
    x_second(3)
    x_second(5)
    x_second(4)
    y_first(1)
    x_second(2)
    x_third(3)
    x_third(5)
    sum_stage(1, 1)
    y_first(0)
    x_third(4)
    x_third(2)
    x_last(3)
    y_second(1)
    y_second(0)
    x_last(5)
    sum_stage(1, 2)
    x_last(4)
    y_last(1)
    x_last(2)

    loss = sum_stage(1, 3) / count_tile
    loss_ref[0, 0] = loss[0, 0]
    y_last(0)
    for copy in sent:
        copy.wait_send()
    for kind in range(4):
        for j in range(YC):
            y_copy(j, kind).wait_send()
        for j in range(YC, CHUNKS):
            x_copy(j, kind).wait_send()


def local(hidden, targets, lengths, head):
    bf16, f32, i32 = jnp.bfloat16, jnp.float32, jnp.int32
    vmem = pl.BlockSpec(memory_space=pltpu.VMEM)
    smem = pl.BlockSpec(memory_space=pltpu.SMEM)
    dma = pltpu.SemaphoreType.DMA
    grad, loss = pl.pallas_call(
        kernel,
        out_shape=(
            jax.ShapeDtypeStruct((2, SUB, WIDTH), bf16),
            jax.ShapeDtypeStruct((1, 1), f32),
        ),
        in_specs=[vmem, vmem, smem, vmem],
        out_specs=(vmem, smem),
        scratch_shapes=[
            pltpu.VMEM((WIDTH, LEVELS), bf16),
            pltpu.VMEM((2, 8, SUB, WIDTH), bf16),
            pltpu.VMEM((8, 1, HOME), i32),
            pltpu.VMEM((ROWS, LEVELS), f32),
            pltpu.VMEM((ROWS, LEVELS), bf16),
            pltpu.VMEM((CHUNKS, 4, 2, SUB, CHUNK), bf16),
            pltpu.VMEM((XC, 2, SUB, CHUNK), bf16),
            pltpu.VMEM((XC, 2, SUB, CHUNK), bf16),
            pltpu.VMEM((XC, 2, SUB, CHUNK), bf16),
            pltpu.VMEM((XC, 2, SUB, CHUNK), bf16),
            pltpu.VMEM((XC, SUB, CHUNK), bf16),
            pltpu.VMEM((XC, SUB, CHUNK), bf16),
            pltpu.VMEM((YC, 4, SUB, CHUNK), bf16),
            pltpu.VMEM((YC, 2, SUB, CHUNK), bf16),
            pltpu.VMEM((YC, SUB, CHUNK), bf16),
            pltpu.VMEM((YC, SUB, CHUNK), bf16),
            pltpu.VMEM((YC, SUB, CHUNK), bf16),
            pltpu.VMEM((YC, SUB, CHUNK), bf16),
            pltpu.VMEM((2, 8, 2, 8, 128), f32),
            pltpu.VMEM((8, 2, 8, 128), f32),
            pltpu.VMEM((2, 8, 128), f32),
            pltpu.VMEM((2, 12, 8, 128), f32),
            dma((2, 4, 3)), dma((2, 4, 3)),
            dma((10,)), dma((10,)),
            dma((35,)), dma((35,)),
            dma((9,)), dma((9,)),
            dma((7,)), dma((7,)),
            dma((3, 7)), dma((3, 7)),
            dma((2, 9)), dma((2, 9)),
            dma((4, XC)), dma((4, XC)),
            dma((4, YC)), dma((4, YC)),
            dma((3,)),
        ],
        compiler_params=pltpu.CompilerParams(
            collective_id=0, has_side_effects=True, vmem_limit_bytes=58 * 2**20
        ),
    )(hidden.reshape(2, SUB, WIDTH), targets.reshape(1, HOME), lengths, head)
    return grad.reshape(HOME, WIDTH), loss.reshape(())


def solution(mesh):
    torus = Mesh(mesh.devices.reshape(SIZES), AXES)
    return jax.shard_map(
        local,
        mesh=torus,
        in_specs=(P(DP + VOCAB, None), P(DP + VOCAB), P(DP), P(DP, VOCAB)),
        out_specs=(P(DP + VOCAB, None), P()),
        check_vma=False,
    )
```

```python
import jax
import jax.numpy as jnp
from jax import lax
from jax.experimental import pallas as pl
from jax.experimental.pallas import tpu as pltpu
from jax.sharding import Mesh
from jax.sharding import PartitionSpec as P

AXES = ("yh", "z", "c", "x", "yl")
SIZES = (2, 8, 2, 4, 2)
DP = ("yh", "z", "c")
VOCAB = ("x", "yl")
MESH = pl.DeviceIdType.MESH

WIDTH = 3072
LEVELS = 2048
HOME = 64
ROWS = 512
HEAD_ROWS = 96
PART = 48
HALF = LEVELS // 2
SUB = 32
CHUNKS = 6
CHUNK = WIDTH // 3
QUAD = 768
XC, YC = 4, 2
HALF_OF = (1, 0, 1, 0, 1, 0)
COLUMN_OF = (2, 2, 0, 1, 1, 0)
TURN = (-1, 1, -1, 1, -1, 1)


def kernel(
    hid_ref, tgt_ref, len_ref, head_ref, grad_ref, loss_ref,
    H, X, A, L, G, PT, XR1, XR2, XR3, XS2, SY, YR, YF, SA, YR1, YR2, YR3, YS2, ST, HT, LS, SB,
    zs, zr, ys, yr, cs, cr, hs, hr, as_, ar, ts, tr, ss, sr, xs, xr, ws, wr, ls,
):
    yh, z, c, x, yl = (lax.axis_index(name) for name in AXES)
    oyh, oc, oyl = 1 - yh, 1 - c, 1 - yl
    me = x * 2 + yl

    def remote(src, dst, send, recv, **device):
        return pltpu.make_async_remote_copy(
            src_ref=src, dst_ref=dst, send_sem=send, recv_sem=recv,
            device_id=device, device_id_type=MESH,
        )

    def zdev(d):
        return lax.rem(z + d + 8, 8)

    def xdev(d):
        return lax.rem(x + d + 4, 4)

    vocab_peers = [(dx, dy) for dx in range(4) for dy in range(2) if dx or dy]

    def vpeer(dx, dy):
        return dict(x=xdev(dx), yl=lax.rem(yl + dy, 2))

    def vindex(dx, dy):
        return xdev(-dx) * 2 + lax.rem(yl + dy, 2)

    barrier = pltpu.get_barrier_semaphore()
    peers = [dict(c=oc), dict(yh=oyh)]
    peers += [dict(z=zdev(d)) for d in range(1, 8)]
    peers += [vpeer(dx, dy) for dx, dy in vocab_peers]
    for device in peers:
        pl.semaphore_signal(barrier, 1, device_id=device, device_id_type=MESH)

    def row0(ring, zz, cc):
        return ring * 1536 + zz * 192 + cc * 96

    def head_at(ring, zz, cc, start, size, lanes=None):
        rows = pl.ds(pl.multiple_of(row0(ring, zz, cc) + start, 16), size)
        if lanes is None:
            return H.at[rows, :]
        return H.at[rows, pl.ds(lanes * HALF, HALF)]

    own_copies = [
        pltpu.make_async_copy(head_ref, head_at(yh, z, c, 0, HEAD_ROWS), ls.at[0]),
        pltpu.make_async_copy(hid_ref, X.at[:, me], ls.at[1]),
        pltpu.make_async_copy(tgt_ref, A.at[me], ls.at[2]),
    ]
    for copy in own_copies:
        copy.start()
    SB[0, 0] = jnp.full((8, 128), len_ref[0], jnp.int32).astype(jnp.float32)
    pl.semaphore_wait(barrier, len(peers))

    sent = []

    def send(copy):
        copy.start()
        sent.append(copy)

    def sum_copy(k, stage, d=0):
        if stage == 0:
            return remote(SB.at[k, 0], SB.at[k, 1], ss.at[k, 0], sr.at[k, 0], c=oc)
        if stage == 1:
            return remote(SB.at[k, 2], SB.at[k, 3], ss.at[k, 1], sr.at[k, 1], yh=oyh)
        return remote(
            SB.at[k, 4 + z], SB.at[k, 4 + z], ss.at[k, 1 + d], sr.at[k, 1 + d], z=zdev(d)
        )

    def sum_stage(k, stage):
        if stage == 1:
            sum_copy(k, 0).wait_recv()
            SB[k, 2] = SB[k, 0] + SB[k, 1]
            sum_copy(k, 1).start()
        elif stage == 2:
            sum_copy(k, 1).wait_recv()
            SB[k, 4 + z] = SB[k, 2] + SB[k, 3]
            for d in range(1, 8):
                sum_copy(k, 2, d).start()
        elif stage == 3:
            for d in range(1, 8):
                remote(
                    SB.at[k, 4 + z], SB.at[k, 4 + zdev(-d)], ss.at[k, 1 + d], sr.at[k, 1 + d], z=zdev(d)
                ).wait_recv()
            total = SB[k, 4]
            for n in range(1, 8):
                total = total + SB[k, 4 + n]
            for stage_ in range(2):
                sum_copy(k, stage_).wait_send()
            for d in range(1, 8):
                sum_copy(k, 2, d).wait_send()
            return total

    DIRS = (1, -1)
    B, OWN_A, PEER_A = 0, 1, 2

    def item_at(item, zz, cc, lanes=None):
        if item == B:
            return head_at(yh, zz, cc, PART, PART, lanes)
        return head_at(yh if item == OWN_A else oyh, zz, cc, 0, PART, lanes)

    def lanes_of(step, dr):
        return None if step < 4 else (0 if dr == 0 else 1)

    def z_send(item, step, dr, src=None):
        zz = zdev(-DIRS[dr] * (step - 1))
        there = item_at(item, zz, c, lanes_of(step, dr))
        send(remote(
            there if src is None else src, there,
            zs.at[dr, step - 1, item], zr.at[dr, step - 1, item], z=zdev(DIRS[dr]),
        ))

    def z_wait(item, step, dr):
        here = item_at(item, zdev(-DIRS[dr] * step), c, lanes_of(step, dr))
        remote(
            here, here, zs.at[dr, step - 1, item], zr.at[dr, step - 1, item], z=zdev(DIRS[dr])
        ).wait_recv()
        return here

    def c_send(index, ref, src=None):
        send(remote(ref if src is None else src, ref, cs.at[index], cr.at[index], c=oc))

    def c_wait(index, ref):
        remote(ref, ref, cs.at[index], cr.at[index], c=oc).wait_recv()

    def c_index(item, step, dr):
        return 1 + (dr * 4 + step - 1) * 3 + item

    def y_send(index, ref, src=None):
        send(remote(ref if src is None else src, ref, ys.at[index], yr.at[index], yh=oyh))

    def y_wait(index, ref):
        remote(ref, ref, ys.at[index], yr.at[index], yh=oyh).wait_recv()

    def y_index(step, dr):
        return 2 + dr * 4 + step - 1

    def peer_b(step, dr, cc):
        return head_at(oyh, zdev(-DIRS[dr] * step), cc, PART, PART, lanes_of(step, dr))

    def hid_at(v, half=None):
        return X.at[:, v] if half is None else X.at[half, v]

    sum_copy(0, 0).start()
    for n, (dx, dy) in enumerate(vocab_peers):
        send(remote(tgt_ref, A.at[me], as_.at[n], ar.at[n], **vpeer(dx, dy)))
    own_a, own_b = head_ref.at[pl.ds(0, PART), :], head_ref.at[pl.ds(PART, PART), :]
    y_send(0, head_at(yh, z, c, 0, PART), own_a)
    for item, own in ((B, own_b), (OWN_A, own_a)):
        for dr in range(2):
            z_send(item, 1, dr, own)
    for dr in range(2):
        send(remote(hid_ref, hid_at(me), hs.at[1 + dr], hr.at[1 + dr], x=xdev(DIRS[dr])))
    y_send(1, head_at(yh, z, c, PART, PART), own_b)
    send(remote(hid_ref, hid_at(me), hs.at[0], hr.at[0], yl=oyl))
    c_send(0, head_at(yh, z, c, 0, HEAD_ROWS), head_ref)

    def pass_on(items, step):
        for item in items:
            for dr in range(2):
                here = z_wait(item, step, dr)
                if step < 4:
                    z_send(item, step + 1, dr)
                if item == B:
                    y_send(y_index(step, dr), here)
                c_send(c_index(item, step, dr), here)

    def take_y(step):
        for dr in range(2):
            ref = peer_b(step, dr, c)
            y_wait(y_index(step, dr), ref)
            c_send(27 + dr * 4 + step - 1, ref)

    def take_c(step, own):
        for dr in range(2):
            for item in (B, OWN_A) if own else (PEER_A,):
                c_wait(
                    c_index(item, step, dr),
                    item_at(item, zdev(-DIRS[dr] * step), oc, lanes_of(step, dr)),
                )
            if not own:
                c_wait(27 + dr * 4 + step - 1, peer_b(step, dr, oc))

    def hid_pass(kind):
        for dr in range(2):
            v = xdev(-DIRS[dr]) * 2 + (yl if kind == 0 else oyl)
            ref = hid_at(v)
            n = 1 + 2 * kind + dr
            remote(ref, ref, hs.at[n], hr.at[n], x=xdev(DIRS[dr])).wait_recv()
            half = hid_at(v, dr)
            n = 5 + 2 * kind + dr
            send(remote(half, half, hs.at[n], hr.at[n], x=xdev(DIRS[dr])))

    def hid_far(kind):
        for dr in range(2):
            half = hid_at(xdev(2) * 2 + (yl if kind == 0 else oyl), dr)
            n = 5 + 2 * kind + dr
            remote(half, half, hs.at[n], hr.at[n], x=xdev(DIRS[dr])).wait_recv()

    def multiply(quad, ring, fresh=False, half=None):
        start = pl.multiple_of(ring * 1536 + quad * QUAD, 256)
        halves = slice(0, 2) if half is None else slice(half, half + 1)
        rows = slice(halves.start * 256, halves.stop * 256)
        width = 512 if half is None else 1024

        def tile(n, carry):
            at = pl.ds(pl.multiple_of(n * width, width), width)
            part = jnp.dot(
                X[halves, :, :, pl.ds(start, QUAD)].reshape(-1, QUAD),
                H[pl.ds(start, QUAD), at],
                preferred_element_type=jnp.float32,
            )
            if fresh:
                L[rows, at] = part
            else:
                L[rows, at] += part
            return carry

        lax.fori_loop(0, LEVELS // width, tile, 0)

    near = lax.div(z, 4)
    far = 1 - near

    pass_on((B,), 1)
    ref = head_at(oyh, z, c, 0, PART)
    y_wait(0, ref)
    for dr in range(2):
        z_send(PEER_A, 1, dr)
    c_send(25, ref)
    pass_on((OWN_A,), 1)
    sum_stage(0, 1)
    hid_pass(0)
    ref = head_at(oyh, z, c, PART, PART)
    y_wait(1, ref)
    c_send(26, ref)
    pass_on((B,), 2)
    hid_peer = hid_at(x * 2 + oyl)
    remote(hid_peer, hid_peer, hs.at[0], hr.at[0], yl=oyl).wait_recv()
    for dr in range(2):
        send(remote(hid_peer, hid_peer, hs.at[3 + dr], hr.at[3 + dr], x=xdev(DIRS[dr])))
    pass_on((PEER_A,), 1)
    pass_on((OWN_A,), 2)
    take_y(1)
    sum_stage(0, 2)
    pass_on((B,), 3)
    hid_pass(1)
    pass_on((PEER_A,), 2)
    pass_on((OWN_A,), 3)
    take_y(2)
    pass_on((B,), 4)
    for copy in own_copies:
        copy.wait()
    for n, (dx, dy) in enumerate(vocab_peers):
        there = A.at[vindex(dx, dy)]
        remote(tgt_ref, there, as_.at[n], ar.at[n], **vpeer(dx, dy)).wait_recv()
    c_wait(0, head_at(yh, z, oc, 0, HEAD_ROWS))
    hid_far(0)
    hid_far(1)
    for step in (1, 2, 3):
        take_c(step, True)
    multiply(near, yh, True)
    pass_on((PEER_A,), 3)
    pass_on((OWN_A,), 4)
    take_y(3)
    take_c(4, True)
    multiply(far, yh)
    pass_on((PEER_A,), 4)
    c_wait(25, head_at(oyh, z, oc, 0, PART))
    c_wait(26, head_at(oyh, z, oc, PART, PART))
    for step in (1, 2, 3):
        take_c(step, False)
    multiply(near, oyh)
    take_y(4)
    count_tile = sum_stage(0, 3)
    take_c(4, False)

    base = me * LEVELS
    lane = lax.broadcasted_iota(jnp.int32, (SUB, 128), 1)
    eye = lane == lax.broadcasted_iota(jnp.int32, (SUB, 128), 0)
    level = lax.broadcasted_iota(jnp.int32, (SUB, LEVELS), 1)
    place64 = lax.broadcasted_iota(jnp.int32, (SUB, HOME), 1)

    def to_row(column):
        return jnp.sum(jnp.where(eye, column, 0.0), axis=0, keepdims=True)

    def to_column(row):
        return jnp.sum(jnp.where(eye, row, 0.0), axis=1, keepdims=True)

    def target_of(half, v):
        row = A[v].astype(jnp.float32)
        here = place64 == lax.broadcasted_iota(jnp.int32, (SUB, HOME), 0) + half * SUB
        column = jnp.sum(jnp.where(here, row, 0.0), axis=1, keepdims=True)
        return column.astype(jnp.int32) - base

    def rows_of(half, v):
        return pl.ds(pl.multiple_of(half * 256 + v * SUB, SUB), SUB)

    def stat_copy(half, n, who):
        ref = ST.at[half, who] if half < 2 else HT.at[who]
        mine = ST.at[half, me] if half < 2 else HT.at[me]
        return remote(mine, ref, ts.at[half, n], tr.at[half, n], **vpeer(*vocab_peers[n]))

    def stat_send(half):
        for n in range(7):
            send(stat_copy(half, n, me))

    def stat_wait(half):
        for n, (dx, dy) in enumerate(vocab_peers):
            stat_copy(half, n, vindex(dx, dy)).wait_recv()

    def statistics(half):
        def block(v, carry):
            logits = L[rows_of(half, v), :]
            top = jnp.max(logits, axis=1, keepdims=True)
            total = jnp.sum(jnp.exp(logits - top), axis=1, keepdims=True)
            ST[half, me, 0, pl.ds(v, 1), :] = to_row(top)
            ST[half, me, 1, pl.ds(v, 1), :] = to_row(total)
            return carry

        for v in range(8):
            block(v, 0)
        stat_send(half)

    for half in range(2):
        multiply(far, oyh, half=half)
        statistics(half)

    def hits(half):
        def block(v, carry):
            found = jnp.where(level == target_of(half, v), L[rows_of(half, v), :], 0.0)
            HT[me, half, pl.ds(v, 1), :] = to_row(jnp.sum(found, axis=1, keepdims=True))
            return carry

        for v in range(8):
            block(v, 0)

    hits(0)
    hits(1)
    stat_send(2)

    length = len_ref[0]
    count = count_tile[0:1, 0:1]

    def gradient(half):
        stat_wait(half)
        top = ST[half, 0, 0]
        for v in range(1, 8):
            top = jnp.maximum(top, ST[half, v, 0])
        total = jnp.zeros((8, 128), jnp.float32)
        for v in range(8):
            total = total + ST[half, v, 1] * jnp.exp(ST[half, v, 0] - top)
        LS[half] = top + jnp.log(total)

        def block(v, carry):
            place = v * HOME + half * SUB + lax.broadcasted_iota(jnp.int32, (SUB, 1), 0)
            weight = jnp.where(place < length, 1.0, 0.0) / count
            share = jnp.exp(L[rows_of(half, v), :] - to_column(LS[half, pl.ds(v, 1), :]))
            share = share - jnp.where(level == target_of(half, v), 1.0, 0.0)
            G[rows_of(half, v), :] = (weight * share).astype(jnp.bfloat16)
            return carry

        for v in range(8):
            block(v, 0)

    def loss_start():
        stat_wait(2)
        lane8 = lax.broadcasted_iota(jnp.int32, (8, 128), 1)
        block8 = lax.broadcasted_iota(jnp.int32, (8, 128), 0)
        row_loss = jnp.zeros((8, 128), jnp.float32)
        for half in range(2):
            hit = HT[0, half]
            for v in range(1, 8):
                hit = hit + HT[v, half]
            counted = (lane8 < SUB) & (block8 * HOME + half * SUB + lane8 < length)
            row_loss = row_loss + jnp.where(counted, LS[half] - hit, 0.0)
        clip_loss = jnp.sum(jnp.sum(row_loss, axis=1, keepdims=True), axis=0, keepdims=True)
        SB[1, 0] = jnp.broadcast_to(clip_loss, (8, 128))
        sum_copy(1, 0).start()

    gradient(0)

    def f32(value):
        return value.astype(jnp.float32)

    def turn(j):
        return TURN[j]

    def columns(j):
        return pl.ds(COLUMN_OF[j] * CHUNK, CHUNK)

    def compute(j):
        product = lax.dot_general(
            G[pl.ds(HALF_OF[j] * 256, 256), :], H[columns(j), :], (((1,), (1,)), ((), ())),
            preferred_element_type=jnp.float32,
        )
        PT[j] = product.astype(jnp.bfloat16).reshape(4, 2, SUB, CHUNK)

    def write(j, value):
        grad_ref[HALF_OF[j], :, columns(j)] = value.astype(jnp.bfloat16)

    def y_copy(j, kind):
        d = turn(j)
        if kind == 0:
            return remote(PT.at[j, :, oyl], YF.at[j], ws.at[0, j], wr.at[0, j], yl=oyl)
        if kind == 1:
            return remote(SA.at[j, 0], YR1.at[j], ws.at[1, j], wr.at[1, j], x=xdev(d))
        if kind == 2:
            return remote(SA.at[j, 1], YR2.at[j], ws.at[2, j], wr.at[2, j], x=xdev(-d))
        return remote(YS2.at[j], YR3.at[j], ws.at[3, j], wr.at[3, j], x=xdev(d))

    def y_sum(j, xx):
        return f32(PT[j, xx, yl]) + f32(YF[j, xx])

    def y_first(j):
        y_copy(j, 0).wait_recv()
        SA[j, 0] = y_sum(j, xdev(2)).astype(jnp.bfloat16)
        SA[j, 1] = y_sum(j, xdev(-turn(j))).astype(jnp.bfloat16)
        y_copy(j, 1).start()
        y_copy(j, 2).start()

    def y_second(j):
        y_copy(j, 1).wait_recv()
        YS2[j] = (y_sum(j, xdev(turn(j))) + f32(YR1[j])).astype(jnp.bfloat16)
        y_copy(j, 3).start()

    def y_last(j):
        y_copy(j, 2).wait_recv()
        y_copy(j, 3).wait_recv()
        write(j, y_sum(j, x) + f32(YR2[j]) + f32(YR3[j]))

    def x_copy(j, kind):
        d, k = turn(j), j - YC
        if kind == 0:
            return remote(PT.at[j, xdev(2)], XR1.at[k], xs.at[0, k], xr.at[0, k], x=xdev(d))
        if kind == 1:
            return remote(PT.at[j, xdev(-d)], XR2.at[k], xs.at[1, k], xr.at[1, k], x=xdev(-d))
        if kind == 2:
            return remote(XS2.at[k], XR3.at[k], xs.at[2, k], xr.at[2, k], x=xdev(d))
        return remote(SY.at[k], YR.at[k], xs.at[3, k], xr.at[3, k], yl=oyl)

    def x_first(j):
        x_copy(j, 0).start()
        x_copy(j, 1).start()

    def x_second(j):
        k = j - YC
        x_copy(j, 0).wait_recv()
        XS2[k] = (f32(PT[j, xdev(turn(j))]) + f32(XR1[k])).astype(jnp.bfloat16)
        x_copy(j, 2).start()

    def x_sum(j, which):
        k = j - YC
        return f32(PT[j, x, which]) + f32(XR2[k, which]) + f32(XR3[k, which])

    def x_third(j):
        k = j - YC
        x_copy(j, 1).wait_recv()
        x_copy(j, 2).wait_recv()
        SY[k] = x_sum(j, oyl).astype(jnp.bfloat16)
        x_copy(j, 3).start()

    def x_last(j):
        x_copy(j, 3).wait_recv()
        write(j, x_sum(j, yl) + f32(YR[j - YC]))

    compute(3)
    x_first(3)
    compute(5)
    x_first(5)
    gradient(1)
    compute(0)
    y_copy(0, 0).start()
    compute(4)
    x_first(4)
    compute(2)
    x_first(2)
    compute(1)
    y_copy(1, 0).start()
    loss_start()
    x_second(5)
    x_second(4)
    x_second(3)
    x_second(2)
    y_first(0)
    y_first(1)
    x_third(5)
    sum_stage(1, 1)
    x_third(4)
    x_third(3)
    x_third(2)
    y_second(0)
    y_second(1)
    x_last(5)
    x_last(4)
    sum_stage(1, 2)
    y_last(0)
    x_last(3)
    x_last(2)

    loss = sum_stage(1, 3) / count_tile
    loss_ref[0, 0] = loss[0, 0]
    y_last(1)
    for copy in sent:
        copy.wait_send()
    for kind in range(4):
        for j in range(YC):
            y_copy(j, kind).wait_send()
        for j in range(YC, CHUNKS):
            x_copy(j, kind).wait_send()


def local(hidden, targets, lengths, head):
    bf16, f32, i32 = jnp.bfloat16, jnp.float32, jnp.int32
    vmem = pl.BlockSpec(memory_space=pltpu.VMEM)
    smem = pl.BlockSpec(memory_space=pltpu.SMEM)
    dma = pltpu.SemaphoreType.DMA
    grad, loss = pl.pallas_call(
        kernel,
        out_shape=(
            jax.ShapeDtypeStruct((2, SUB, WIDTH), bf16),
            jax.ShapeDtypeStruct((1, 1), f32),
        ),
        in_specs=[vmem, vmem, smem, vmem],
        out_specs=(vmem, smem),
        scratch_shapes=[
            pltpu.VMEM((WIDTH, LEVELS), bf16),
            pltpu.VMEM((2, 8, SUB, WIDTH), bf16),
            pltpu.VMEM((8, 1, HOME), i32),
            pltpu.VMEM((ROWS, LEVELS), f32),
            pltpu.VMEM((ROWS, LEVELS), bf16),
            pltpu.VMEM((CHUNKS, 4, 2, SUB, CHUNK), bf16),
            pltpu.VMEM((XC, 2, SUB, CHUNK), bf16),
            pltpu.VMEM((XC, 2, SUB, CHUNK), bf16),
            pltpu.VMEM((XC, 2, SUB, CHUNK), bf16),
            pltpu.VMEM((XC, 2, SUB, CHUNK), bf16),
            pltpu.VMEM((XC, SUB, CHUNK), bf16),
            pltpu.VMEM((XC, SUB, CHUNK), bf16),
            pltpu.VMEM((YC, 4, SUB, CHUNK), bf16),
            pltpu.VMEM((YC, 2, SUB, CHUNK), bf16),
            pltpu.VMEM((YC, SUB, CHUNK), bf16),
            pltpu.VMEM((YC, SUB, CHUNK), bf16),
            pltpu.VMEM((YC, SUB, CHUNK), bf16),
            pltpu.VMEM((YC, SUB, CHUNK), bf16),
            pltpu.VMEM((2, 8, 2, 8, 128), f32),
            pltpu.VMEM((8, 2, 8, 128), f32),
            pltpu.VMEM((2, 8, 128), f32),
            pltpu.VMEM((2, 12, 8, 128), f32),
            dma((2, 4, 3)), dma((2, 4, 3)),
            dma((10,)), dma((10,)),
            dma((35,)), dma((35,)),
            dma((9,)), dma((9,)),
            dma((7,)), dma((7,)),
            dma((3, 7)), dma((3, 7)),
            dma((2, 9)), dma((2, 9)),
            dma((4, XC)), dma((4, XC)),
            dma((4, YC)), dma((4, YC)),
            dma((3,)),
        ],
        compiler_params=pltpu.CompilerParams(
            collective_id=0, has_side_effects=True, vmem_limit_bytes=58 * 2**20
        ),
    )(hidden.reshape(2, SUB, WIDTH), targets.reshape(1, HOME), lengths, head)
    return grad.reshape(HOME, WIDTH), loss.reshape(())


def solution(mesh):
    torus = Mesh(mesh.devices.reshape(SIZES), AXES)
    return jax.shard_map(
        local,
        mesh=torus,
        in_specs=(P(DP + VOCAB, None), P(DP + VOCAB), P(DP), P(DP, VOCAB)),
        out_specs=(P(DP + VOCAB, None), P()),
        check_vma=False,
    )
```
